128 devices in a mesh: slab: 32 (over z, x, core), pen: 4 (over y).
Axes of the slice: x: 4, y: 4, z: 4, core: 2. Of those that a mesh axis runs over, the one named last changes fastest.
Arguments:
- pressure: float32 [512, 512, 512], P('slab', 'pen'), may hold values from -6 to 6
- previous: float32 [512, 512, 512], P('slab', 'pen'), may hold values from -6 to 6
- speed_ratio: float32 [512, 512, 512], P('slab', 'pen'), may hold values from 0.25 to 1
- traces: float32 [2, 2048], P(None, ('slab', 'pen')), may hold values from -6 to 6
- sensor_voxels: int32 [3, 2048], replicated, may hold values from 0 to 511, as said below
- trace_column: int32 [2048], replicated, may hold values from 0 to 2047, each once
Outputs:
- final_pressure: float32 [512, 512, 512], P('slab', 'pen')
- prior_pressure: float32 [512, 512, 512], P('slab', 'pen')
The draws below stay inside these ranges and needn't reach their ends.
Inputs may be any that keep to these rules, and one draw needn't show every extreme that they name: `sensor_voxels`: row 0 holds each sensor's z cell (below 512), row 1 its y cell (below 512), row 2 its x cell (below 512); no two sensors share a y, x pair. `trace_column`: each of the 2048 trace columns belongs to exactly one sensor.
All inputs are finite; a program needn't handle non-finite values.
Results may differ from the reference program's by a relative error of at most 0.0001.
Values sent between devices are 32-bit elements; how exact they have to be, the bound alone decides.
No kernel may reach another device: no remote copies, remote signals or barrier semaphores. Data moves between devices by JAX's collectives and lax.ppermute only.
A program may use at most 128 MiB of HBM per device.

```python
import math
import jax
import jax.numpy as jnp

NX = 512
NY = 512
NZ = 512
STEPS = 2
SENSORS = 2048


def draw_sensor_voxels(key, part):
    depth_key, plane_key = jax.random.split(jax.random.fold_in(key, 11))
    picks = jax.random.randint(depth_key, (3, SENSORS), 0, NZ)
    zcoord = jnp.min(picks, axis=0)
    chosen = jax.random.permutation(plane_key, NY * NX)[:SENSORS]
    return jnp.stack([zcoord, chosen // NX, chosen % NX]).astype(jnp.int32)


def levels(key, extent, cuts, low, high):
    level, own = 1.0, jax.random.fold_in(key, 6)
    for position, shards_of in cuts:
        steps = jnp.exp(jax.random.uniform(jax.random.fold_in(own, position), (shards_of,), jnp.float32, low / len(cuts), high / len(cuts)))
        level = level * jnp.repeat(steps, extent[position] // shards_of).reshape([-1 if axis == position else 1 for axis in range(len(extent))])
    return level


def noise(stream_key, extent, scale, most, pieces=(), kind=jnp.bfloat16):
    drawn = jax.random.normal(stream_key, extent, jnp.float32) * scale
    if len(pieces) > 0:
        drawn = levels(stream_key, extent, pieces, -0.22, 0.18) * drawn
    return jnp.clip(drawn, min=-most, max=most).astype(kind)


def setup_inputs(seed: int = 0) -> dict:
    key_of = jax.random.split(jax.random.key(seed), 7)
    return {
        "pressure": noise(key_of[0], (NZ, NY, NX), 1.0, 6.0, ((0, 32), (1, 4)), jnp.float32),
        "previous": noise(key_of[1], (NZ, NY, NX), 1.0, 6.0, ((0, 32), (1, 4)), jnp.float32),
        "speed_ratio": jnp.clip(jnp.exp(math.log(1.0) - 1.3862944 * jax.random.uniform(key_of[2], (NZ, NY, NX), jnp.float32) ** levels(key_of[2], (NZ, NY, NX), ((0, 32), (1, 4)), -0.2, 0.2)), 0.25, 1.0),
        "traces": noise(key_of[3], (STEPS, SENSORS), 1.0, 6.0, ((1, 128),), jnp.float32),
        "sensor_voxels": draw_sensor_voxels(jax.random.fold_in(key_of[6], 71), 0),
        "trace_column": jax.random.permutation(key_of[5], SENSORS).astype(jnp.int32),
    }


def squared_freq(length):
    indices = jnp.arange(length, dtype=jnp.int32)
    signed_index = jnp.where(2 * indices > length, indices - length, indices)
    angular = signed_index.astype(jnp.float32) * (2.0 * math.pi / length)
    return angular * angular

def reference(pressure, previous, speed_ratio, traces, sensor_voxels, trace_column):
    freq_z = squared_freq(NZ)
    freq_y = squared_freq(NY)
    half_x = jnp.arange(NX // 2 + 1, dtype=jnp.int32).astype(jnp.float32) * (2.0 * math.pi / NX)
    freq_x = half_x * half_x
    total = freq_z[:, None, None] + freq_y[None, :, None] + freq_x[None, None, :]
    symbol = -4.0 * jnp.square(jnp.sin(0.25 * jnp.sqrt(total)))
    zcell = sensor_voxels[0]
    ycell = sensor_voxels[1]
    xcell = sensor_voxels[2]
    for step_index in range(STEPS):
        values = traces[step_index][trace_column]
        current = pressure.at[zcell, ycell, xcell].set(values)
        spectrum = jnp.fft.rfftn(current)
        update = jnp.fft.irfftn(spectrum * symbol, s=current.shape).astype(jnp.float32)
        following = 2.0 * current - previous + speed_ratio * update
        previous = current
        pressure = following
    return (pressure, previous)
```

```python
import functools
import math

import jax
import jax.numpy as jnp
import numpy as np
from jax import lax
from jax.experimental import pallas as pl
from jax.experimental.pallas import tpu as pltpu
from jax.sharding import Mesh
from jax.sharding import PartitionSpec as P

NX = 512
NY = 512
NZ = 512
HALF = 256
SENSORS = 2048
SLAB = ("slab_0", "slab_1", "slab_2")
SLAB_PEN = ("slab_0", "slab_1", "slab_2", "pen")
HALF_CFL = 0.25
MIB = 1024 * 1024
F32 = jnp.float32
BF16 = jnp.bfloat16


def half_tables():
    m = np.arange(HALF)[:, None]
    n = np.arange(HALF)[None, :]
    parts = []
    for freq in (2 * m, 2 * m + 1):
        angle = (freq * n % 512) * (2.0 * math.pi / 512)
        parts.append(np.cos(angle) + np.sin(angle))
    even, odd = parts
    stack = []
    for table in (even, odd, odd.T):
        high = table.astype(BF16)
        low = (table - high.astype(np.float64)).astype(BF16)
        stack += [high, low]
    return np.stack(stack)


EVEN, ODD, ODD_T = 0, 2, 4


def split(x):
    high = x.astype(BF16)
    low = (x - high.astype(F32)).astype(BF16)
    return high, low


def split3(x, axis):
    high, low = split(x)
    return jnp.concatenate([high, low, high], axis=axis)


def table3(tab, which, axis):
    high = tab[which]
    return jnp.concatenate([high, high, tab[which + 1]], axis=axis)


def dot(left, right, dims):
    return lax.dot_general(left, right, (dims, ((), ())), preferred_element_type=F32)


def sensor_kernel(offs, vox, tcol, gt, zmap, vmap0, vmap1):
    z = vox[0:1, :] - offs[0]
    y = vox[1:2, :] - offs[1]
    x = vox[2:3, :]
    tile = tcol[...] // 16
    lane = tcol[...] % 16
    inside = (z >= 0) & (z < 16) & (y >= 0) & (y < 128)
    y = jnp.where(inside, y, -1)
    rows128 = lax.broadcasted_iota(jnp.int32, (128, SENSORS), 0)
    pick = (rows128 == tile).astype(F32).astype(BF16)
    g = gt[...]
    g0, g1 = split(g)
    g2 = (g - g0.astype(F32) - g1.astype(F32)).astype(BF16)
    parts = dot(jnp.concatenate([g0, g1, g2], axis=0), pick, ((1,), (0,)))
    spread = parts[0:32] + parts[32:64] + parts[64:96]
    rows16 = lax.broadcasted_iota(jnp.int32, (16, SENSORS), 0)
    here = rows16 == lane
    onrow = rows128 == y
    lhs = [jnp.where(onrow, (z + 1).astype(F32), 0.0).astype(BF16)]
    for t in range(2):
        value = jnp.sum(jnp.where(here, spread[16 * t : 16 * t + 16], 0.0), axis=0, keepdims=True)
        v0 = value.astype(BF16).astype(F32)
        v1 = (value - v0).astype(BF16).astype(F32)
        v2 = value - v0 - v1
        for part in (v0, v1, v2):
            lhs.append(jnp.where(onrow, part, 0.0).astype(BF16))
    columns = lax.broadcasted_iota(jnp.int32, (NX, SENSORS), 0)
    oncol = (columns == x).astype(F32).astype(BF16)
    out = dot(jnp.concatenate(lhs, axis=0), oncol, ((1,), (1,)))
    zmap[...] = out[0:128].astype(jnp.int32) - 1
    vmap0[...] = out[128:256] + out[256:384] + out[384:512]
    vmap1[...] = out[512:640] + out[640:768] + out[768:896]


def forward_x(cur, tab, out):
    flat = cur.reshape(256, NX)
    a, b = flat[:, :HALF], flat[:, HALF:]
    out2 = out.reshape(1024, 128)
    for part, (which, data) in enumerate(((EVEN, a + b), (ODD, a - b))):
        got = dot(table3(tab, which, 1), split3(data, 1), ((1,), (1,)))
        for k in range(2):
            for z in range(2):
                out2[pl.ds(z * 4 + part * 2 + k, 128, stride=8), :] = got[
                    k * 128 : (k + 1) * 128, z * 128 : (z + 1) * 128
                ]


def inverse_x(arr, tab):
    arr2 = arr.reshape(1024, 128)
    halves = []
    for part, which in enumerate((EVEN, ODD)):
        pieces = []
        for z in range(2):
            rows = [arr2[pl.ds(z * 4 + part * 2 + k, 128, stride=8), :] for k in range(2)]
            pieces.append(jnp.concatenate(rows, axis=0))
        data = jnp.concatenate(pieces, axis=1)
        halves.append(dot(split3(data, 0), table3(tab, which, 0), ((0,), (0,))))
    even, odd = halves
    return jnp.concatenate([even + odd, even - odd], axis=1).reshape(2, 128, NX)


def inject(base, zmap, vmap):
    z = lax.broadcasted_iota(jnp.int32, (2, 1, 1), 0) + 2 * pl.program_id(0)
    return jnp.where(zmap[...][None] == z, vmap[...][None], base)


def first_kernel(p, zmap, vmap0, tab, out):
    forward_x(inject(p[...], zmap, vmap0), tab, out)


def middle_kernel(arr, prev, speed, p, zmap, vmap0, vmap1, tab, cur_out, out):
    update = inverse_x(arr, tab)
    now = inject(p[...], zmap, vmap0)
    following = 2.0 * now - prev[...] + speed[...] * update
    cur = inject(following, zmap, vmap1)
    cur_out[...] = cur
    forward_x(cur, tab, out)


def last_kernel(arr, cur, speed, p, zmap, vmap0, tab, final):
    update = inverse_x(arr, tab)
    before = inject(p[...], zmap, vmap0)
    final[...] = 2.0 * cur[...] - before + speed[...] * update


def spectral_kernel(arr, sym, tab, out):
    k = pl.program_id(0)
    pens = [arr[:, p, pl.ds(k, 16, stride=4), :].reshape(512, 128) for p in range(4)]
    a = jnp.concatenate(pens[:2], axis=1)
    b = jnp.concatenate(pens[2:], axis=1)
    back = []
    for part, data in enumerate((a + b, a - b)):
        which = (EVEN, ODD_T)[part]
        x = dot(split3(data, 1), table3(tab, which, 0), ((1,), (0,)))
        top, bottom = x[:HALF], x[HALF:]
        even = dot(table3(tab, EVEN, 1), split3(top + bottom, 0), ((1,), (0,)))
        odd = dot(table3(tab, ODD, 1), split3(top - bottom, 0), ((1,), (0,)))
        cols = pl.ds(part * HALF, HALF)
        even = even * sym[0, pl.ds(0, HALF), cols]
        odd = odd * sym[0, pl.ds(HALF, HALF), cols]
        even = dot(table3(tab, EVEN, 1), split3(even, 0), ((1,), (0,)))
        odd = dot(table3(tab, ODD_T, 1), split3(odd, 0), ((1,), (0,)))
        z = jnp.concatenate([even + odd, even - odd], axis=0)
        back.append(dot(split3(z, 1), table3(tab, (EVEN, ODD)[part], 0), ((1,), (0,))))
    a = back[0] + back[1]
    b = back[0] - back[1]
    for p in range(4):
        piece = (a, b)[p // 2][:, (p % 2) * 128 : (p % 2) * 128 + 128]
        out[:, p, pl.ds(k, 16, stride=4), :] = piece.reshape(32, 16, 128)


def whole(*shape):
    return pl.BlockSpec(shape, lambda i: (0,) * len(shape))


def pairs():
    return pl.BlockSpec((2, 128, NX), lambda i: (i, 0, 0))


def packed():
    return pl.BlockSpec((128, 8, 128), lambda i: (0, i, 0))


def params(mib):
    return pltpu.CompilerParams(vmem_limit_bytes=mib * MIB)


TAB = whole(6, HALF, HALF)
MAP = whole(128, NX)
GRID = jax.ShapeDtypeStruct((16, 128, NX), F32)
WIRE = jax.ShapeDtypeStruct((128, 64, 128), F32)


def squared_freq(indices, length):
    signed_index = jnp.where(2 * indices > length, indices - length, indices)
    angular = signed_index.astype(F32) * (2.0 * math.pi / length)
    return angular * angular


def half_order(rows):
    return jnp.where(rows < HALF, 2 * rows, 2 * (rows - HALF) + 1)


def symbol_of(device):
    rows = jnp.arange(512, dtype=jnp.int32)
    freq = squared_freq(half_order(rows), 512)
    local = jnp.arange(4, dtype=jnp.int32) * 128 + device
    freq_x = squared_freq(half_order(local), NX)
    total = freq[None, :, None] + freq[None, None, :] + freq_x[:, None, None]
    scale = 1.0 / (NX * NY * NZ)
    return -4.0 * jnp.square(jnp.sin(HALF_CFL * jnp.sqrt(total))) * scale


def exchange(array):
    return lax.all_to_all(array, SLAB_PEN, split_axis=0, concat_axis=0, tiled=True)


def on_device(pressure, previous, speed_ratio, traces, sensor_voxels, trace_column):
    slab_index = lax.axis_index(SLAB)
    pen_index = lax.axis_index("pen")
    device = slab_index * 4 + pen_index
    tab = jnp.asarray(half_tables())
    gathered = exchange(jnp.broadcast_to(traces[None], (128, 2, 16)))
    gt = gathered.reshape(128, 32).T
    offs = jnp.stack([slab_index * 16, pen_index * 128]).astype(jnp.int32)
    map_type = jax.ShapeDtypeStruct((128, NX), F32)
    zmap, vmap0, vmap1 = pl.pallas_call(
        sensor_kernel,
        in_specs=[pl.BlockSpec(memory_space=pltpu.SMEM)] + [pl.BlockSpec(memory_space=pltpu.VMEM)] * 3,
        out_shape=(jax.ShapeDtypeStruct((128, NX), jnp.int32), map_type, map_type),
        compiler_params=params(40),
        name="sensors",
    )(offs, sensor_voxels, trace_column.reshape(1, SENSORS), gt)
    sym = symbol_of(device)

    wire = pl.pallas_call(
        first_kernel,
        grid=(8,),
        in_specs=[pairs(), MAP, MAP, TAB],
        out_specs=packed(),
        out_shape=WIRE,
        compiler_params=params(24),
        name="first",
    )(pressure, zmap, vmap0, tab)

    def spectral(arr):
        return pl.pallas_call(
            spectral_kernel,
            grid=(4,),
            in_specs=[whole(32, 4, 64, 128), pl.BlockSpec((1, 512, 512), lambda i: (i, 0, 0)), TAB],
            out_specs=whole(32, 4, 64, 128),
            out_shape=jax.ShapeDtypeStruct((32, 4, 64, 128), F32),
            compiler_params=params(40),
            name="spectral",
        )(arr.reshape(32, 4, 64, 128), sym, tab).reshape(128, 64, 128)

    arr = exchange(spectral(exchange(wire)))
    current, wire = pl.pallas_call(
        middle_kernel,
        grid=(8,),
        in_specs=[packed(), pairs(), pairs(), pairs(), MAP, MAP, MAP, TAB],
        out_specs=(pairs(), packed()),
        out_shape=(GRID, WIRE),
        compiler_params=params(32),
        name="middle",
    )(arr, previous, speed_ratio, pressure, zmap, vmap0, vmap1, tab)
    arr = exchange(spectral(exchange(wire)))
    final = pl.pallas_call(
        last_kernel,
        grid=(8,),
        in_specs=[packed(), pairs(), pairs(), pairs(), MAP, MAP, TAB],
        out_specs=pairs(),
        out_shape=GRID,
        compiler_params=params(32),
        name="last",
    )(arr, current, speed_ratio, pressure, zmap, vmap0, tab)
    return (final, current)


def solution(mesh):
    torus = Mesh(
        mesh.devices.reshape(4, 4, 2, mesh.shape["pen"]), ("slab_0", "slab_1", "slab_2", "pen")
    )
    placed = (
        P(SLAB, "pen", None),
        P(SLAB, "pen", None),
        P(SLAB, "pen", None),
        P(None, SLAB_PEN),
        P(),
        P(),
    )
    return jax.shard_map(
        on_device,
        mesh=torus,
        in_specs=placed,
        out_specs=(P(SLAB, "pen", None), P(SLAB, "pen", None)),
        check_vma=False,
    )
```

```python
import math

import jax
import jax.numpy as jnp
import numpy as np
from jax import lax
from jax.experimental import pallas as pl
from jax.experimental.pallas import tpu as pltpu
from jax.sharding import Mesh
from jax.sharding import PartitionSpec as P

NX = 512
NY = 512
NZ = 512
HALF = 256
SENSORS = 2048
SLAB = ("slab_0", "slab_1", "slab_2")
SLAB_PEN = ("slab_0", "slab_1", "slab_2", "pen")
HALF_CFL = 0.25
MIB = 1024 * 1024
F32 = jnp.float32
BF16 = jnp.bfloat16


def half_tables():
    m = np.arange(HALF)[:, None]
    n = np.arange(HALF)[None, :]
    parts = []
    for freq in (2 * m, 2 * m + 1):
        angle = (freq * n % 512) * (2.0 * math.pi / 512)
        parts.append(np.cos(angle) + np.sin(angle))
    even, odd = parts
    stack = []
    for table in (even, odd, odd.T):
        high = table.astype(BF16)
        low = (table - high.astype(np.float64)).astype(BF16)
        stack += [high, low]
    return np.stack(stack)


EVEN, ODD, ODD_T = 0, 2, 4


def split(x):
    high = x.astype(BF16)
    low = (x - high.astype(F32)).astype(BF16)
    return high, low


def split3(x, axis):
    high, low = split(x)
    return jnp.concatenate([high, low, high], axis=axis)


def table3(tab, which, axis):
    high = tab[which]
    return jnp.concatenate([high, high, tab[which + 1]], axis=axis)


def dot(left, right, dims):
    return lax.dot_general(left, right, (dims, ((), ())), preferred_element_type=F32)


def cell_kernel(offs, vox, zmap):
    z = vox[0:1, :] - offs[0]
    y = vox[1:2, :] - offs[1]
    inside = (z >= 0) & (z < 16) & (y >= 0) & (y < 128)
    y = jnp.where(inside, y, -1)
    rows128 = lax.broadcasted_iota(jnp.int32, (128, SENSORS), 0)
    lhs = jnp.where(rows128 == y, (z + 1).astype(F32), 0.0).astype(BF16)
    columns = lax.broadcasted_iota(jnp.int32, (NX, SENSORS), 0)
    oncol = (columns == vox[2:3, :]).astype(F32).astype(BF16)
    zmap[...] = dot(lhs, oncol, ((1,), (1,))).astype(jnp.int32) - 1


def value_kernel(offs, vox, tcol, gathered, vmap0, vmap1, row0):
    z = vox[0:1, :] - offs[0]
    y = vox[1:2, :] - offs[1]
    tile = (tcol[...] // 16) ^ offs[2]
    lane = tcol[...] % 16
    inside = (z >= 0) & (z < 16) & (y >= 0) & (y < 128)
    y = jnp.where(inside, y, -1)
    rows128 = lax.broadcasted_iota(jnp.int32, (128, SENSORS), 0)
    pick = (rows128 == tile).astype(F32).astype(BF16)
    g = gathered[...].T
    g0, g1 = split(g)
    g2 = (g - g0.astype(F32) - g1.astype(F32)).astype(BF16)
    parts = dot(jnp.concatenate([g0, g1, g2], axis=0), pick, ((1,), (0,)))
    spread = parts[0:32] + parts[32:64] + parts[64:96]
    rows16 = lax.broadcasted_iota(jnp.int32, (16, SENSORS), 0)
    here = rows16 == lane
    onrow = rows128 == y
    lhs = []
    for t in range(2):
        value = jnp.sum(jnp.where(here, spread[16 * t : 16 * t + 16], 0.0), axis=0, keepdims=True)
        if t == 0:
            row0[...] = value
        v0 = value.astype(BF16).astype(F32)
        v1 = (value - v0).astype(BF16).astype(F32)
        v2 = value - v0 - v1
        for part in (v0, v1, v2):
            lhs.append(jnp.where(onrow, part, 0.0).astype(BF16))
    columns = lax.broadcasted_iota(jnp.int32, (NX, SENSORS), 0)
    oncol = (columns == vox[2:3, :]).astype(F32).astype(BF16)
    out = dot(jnp.concatenate(lhs, axis=0), oncol, ((1,), (1,)))
    vmap0[...] = out[0:128] + out[128:256] + out[256:384]
    vmap1[...] = out[384:512] + out[512:640] + out[640:768]


def seed_kernel(vox, weight, out):
    rows = lax.broadcasted_iota(jnp.int32, (512, SENSORS), 0)
    onrow = rows == vox[0:1, :]
    oncol = (rows == vox[1:2, :]).astype(F32).astype(BF16)
    value = weight[pl.ds(pl.program_id(0), 1), :]
    high = value.astype(BF16).astype(F32)
    low = value - high
    lhs = [jnp.where(onrow, part, 0.0).astype(BF16) for part in (high, low)]
    got = dot(jnp.concatenate(lhs, axis=0), oncol, ((1,), (1,)))
    out[0] = got[:512] + got[512:]


def forward_x(cur, tab, out):
    flat = cur.reshape(256, NX)
    a, b = flat[:, :HALF], flat[:, HALF:]
    out2 = out.reshape(1024, 128)
    for part, (which, data) in enumerate(((EVEN, a + b), (ODD, a - b))):
        got = dot(table3(tab, which, 1), split3(data, 1), ((1,), (1,)))
        for k in range(2):
            for z in range(2):
                out2[pl.ds(z * 4 + part * 2 + k, 128, stride=8), :] = got[
                    k * 128 : (k + 1) * 128, z * 128 : (z + 1) * 128
                ]


def inverse_x(arr, tab):
    arr2 = arr.reshape(1024, 128)
    halves = []
    for part, which in enumerate((EVEN, ODD)):
        pieces = []
        for z in range(2):
            rows = [arr2[pl.ds(z * 4 + part * 2 + k, 128, stride=8), :] for k in range(2)]
            pieces.append(jnp.concatenate(rows, axis=0))
        data = jnp.concatenate(pieces, axis=1)
        halves.append(dot(split3(data, 0), table3(tab, which, 0), ((0,), (0,))))
    even, odd = halves
    return jnp.concatenate([even + odd, even - odd], axis=1).reshape(2, 128, NX)


def inject(base, zmap, vmap):
    z = lax.broadcasted_iota(jnp.int32, (2, 1, 1), 0) + 2 * pl.program_id(0)
    return jnp.where(zmap[...][None] == z, vmap[...][None], base)


def first_kernel(p, zmap, tab, out):
    z = lax.broadcasted_iota(jnp.int32, (2, 1, 1), 0) + 2 * pl.program_id(0)
    forward_x(jnp.where(zmap[...][None] == z, 0.0, p[...]), tab, out)


def middle_kernel(arr, prev, speed, p, zmap, vmap0, vmap1, tab, cur_out, out):
    update = inverse_x(arr, tab)
    now = inject(p[...], zmap, vmap0)
    following = 2.0 * now - prev[...] + speed[...] * update
    cur = inject(following, zmap, vmap1)
    cur_out[...] = cur
    forward_x(cur, tab, out)


def last_kernel(arr, cur, speed, p, zmap, vmap0, tab, final):
    update = inverse_x(arr, tab)
    before = inject(p[...], zmap, vmap0)
    final[...] = 2.0 * cur[...] - before + speed[...] * update


def seeded_kernel(arr, seed, sym, tab, out):
    spectral_kernel(arr, sym, tab, out, seed)


def spectral_kernel(arr, sym, tab, out, seed=None):
    k = pl.program_id(0)
    pens = [arr[:, p, pl.ds(k, 16, stride=4), :].reshape(512, 128) for p in range(4)]
    a = jnp.concatenate(pens[:2], axis=1)
    b = jnp.concatenate(pens[2:], axis=1)
    if seed is not None:
        a = a + seed[0, :, :HALF]
        b = b + seed[0, :, HALF:]
    back = []
    for part, data in enumerate((a + b, a - b)):
        which = (EVEN, ODD_T)[part]
        x = dot(split3(data, 1), table3(tab, which, 0), ((1,), (0,)))
        top, bottom = x[:HALF], x[HALF:]
        even = dot(table3(tab, EVEN, 1), split3(top + bottom, 0), ((1,), (0,)))
        odd = dot(table3(tab, ODD, 1), split3(top - bottom, 0), ((1,), (0,)))
        cols = pl.ds(part * HALF, HALF)
        even = even * sym[0, pl.ds(0, HALF), cols]
        odd = odd * sym[0, pl.ds(HALF, HALF), cols]
        even = dot(table3(tab, EVEN, 1), split3(even, 0), ((1,), (0,)))
        odd = dot(table3(tab, ODD_T, 1), split3(odd, 0), ((1,), (0,)))
        z = jnp.concatenate([even + odd, even - odd], axis=0)
        back.append(dot(split3(z, 1), table3(tab, (EVEN, ODD)[part], 0), ((1,), (0,))))
    a = back[0] + back[1]
    b = back[0] - back[1]
    for p in range(4):
        piece = (a, b)[p // 2][:, (p % 2) * 128 : (p % 2) * 128 + 128]
        out[:, p, pl.ds(k, 16, stride=4), :] = piece.reshape(32, 16, 128)


def whole(*shape):
    return pl.BlockSpec(shape, lambda i: (0,) * len(shape))


def pairs():
    return pl.BlockSpec((2, 128, NX), lambda i: (i, 0, 0))


def packed():
    return pl.BlockSpec((128, 8, 128), lambda i: (0, i, 0))


def params(mib):
    return pltpu.CompilerParams(vmem_limit_bytes=mib * MIB)


TAB = whole(6, HALF, HALF)
MAP = whole(128, NX)
GRID = jax.ShapeDtypeStruct((16, 128, NX), F32)
WIRE = jax.ShapeDtypeStruct((128, 64, 128), F32)


def squared_freq(indices, length):
    signed_index = jnp.where(2 * indices > length, indices - length, indices)
    angular = signed_index.astype(F32) * (2.0 * math.pi / length)
    return angular * angular


def half_order(rows):
    return jnp.where(rows < HALF, 2 * rows, 2 * (rows - HALF) + 1)


def local_freq(device):
    return half_order(jnp.arange(4, dtype=jnp.int32) * 128 + device)


def symbol_of(device):
    rows = jnp.arange(512, dtype=jnp.int32)
    freq = squared_freq(half_order(rows), 512)
    freq_x = squared_freq(local_freq(device), NX)
    total = freq[None, :, None] + freq[None, None, :] + freq_x[:, None, None]
    square = total * (HALF_CFL * HALF_CFL)
    ratio = jnp.full_like(square, 1.0 / math.factorial(15) * -1.0)
    for n in (13, 11, 9, 7, 5, 3, 1):
        sign = 1.0 if n % 4 == 1 else -1.0
        ratio = ratio * square + sign / math.factorial(n)
    scale = -4.0 / (NX * NY * NZ)
    return square * ratio * ratio * scale


def exchange(array):
    return lax.all_to_all(array, SLAB_PEN, split_axis=0, concat_axis=0, tiled=True)


def gather_traces(traces):
    state = traces.reshape(1, 32)
    for bit in range(7):
        pairs_of = [(i, i ^ (1 << bit)) for i in range(128)]
        state = jnp.concatenate([state, lax.ppermute(state, SLAB_PEN, pairs_of)], axis=0)
    return state


def step_pair(pressure, previous, speed_ratio, traces, sensor_voxels, trace_column):
    slab_index = lax.axis_index(SLAB)
    pen_index = lax.axis_index("pen")
    device = slab_index * 4 + pen_index
    tab = jnp.asarray(half_tables())
    offs = jnp.stack([slab_index * 16, pen_index * 128, device]).astype(jnp.int32)
    in_smem = pl.BlockSpec(memory_space=pltpu.SMEM)
    in_vmem = pl.BlockSpec(memory_space=pltpu.VMEM)
    zmap = pl.pallas_call(
        cell_kernel,
        in_specs=[in_smem, in_vmem],
        out_specs=in_vmem,
        out_shape=jax.ShapeDtypeStruct((128, NX), jnp.int32),
        compiler_params=params(24),
        name="cells",
    )(offs, sensor_voxels)
    wire = pl.pallas_call(
        first_kernel,
        grid=(8,),
        in_specs=[pairs(), MAP, TAB],
        out_specs=packed(),
        out_shape=WIRE,
        compiler_params=params(24),
        name="first",
    )(pressure, zmap, tab)
    arr = exchange(wire)

    gathered = gather_traces(traces)
    map_type = jax.ShapeDtypeStruct((128, NX), F32)
    vmap0, vmap1, row0 = pl.pallas_call(
        value_kernel,
        in_specs=[in_smem] + [in_vmem] * 3,
        out_specs=(in_vmem,) * 3,
        out_shape=(map_type, map_type, jax.ShapeDtypeStruct((1, SENSORS), F32)),
        compiler_params=params(40),
        name="values",
    )(offs, sensor_voxels, trace_column.reshape(1, SENSORS), gathered)
    angle = (local_freq(device)[:, None] * sensor_voxels[2][None, :] % NX).astype(F32) * (2.0 * math.pi / NX)
    weight = row0 * (jnp.cos(angle) + jnp.sin(angle))
    plane = pl.BlockSpec((1, 512, 512), lambda i: (i, 0, 0))
    seed = pl.pallas_call(
        seed_kernel,
        grid=(4,),
        in_specs=[whole(3, SENSORS), whole(4, SENSORS)],
        out_specs=plane,
        out_shape=jax.ShapeDtypeStruct((4, 512, 512), F32),
        compiler_params=params(32),
        name="seeds",
    )(sensor_voxels, weight)
    sym = symbol_of(device)

    def spectral(arr, *extra):
        return pl.pallas_call(
            seeded_kernel if extra else spectral_kernel,
            grid=(4,),
            in_specs=[whole(32, 4, 64, 128)] + [plane] * (len(extra) + 1) + [TAB],
            out_specs=whole(32, 4, 64, 128),
            out_shape=jax.ShapeDtypeStruct((32, 4, 64, 128), F32),
            compiler_params=params(40),
            name="seeded" if extra else "spectral",
        )(arr.reshape(32, 4, 64, 128), *extra, sym, tab).reshape(128, 64, 128)

    arr = exchange(spectral(arr, seed))
    current, wire = pl.pallas_call(
        middle_kernel,
        grid=(8,),
        in_specs=[packed(), pairs(), pairs(), pairs(), MAP, MAP, MAP, TAB],
        out_specs=(pairs(), packed()),
        out_shape=(GRID, WIRE),
        compiler_params=params(32),
        name="middle",
    )(arr, previous, speed_ratio, pressure, zmap, vmap0, vmap1, tab)
    arr = exchange(spectral(exchange(wire)))
    final = pl.pallas_call(
        last_kernel,
        grid=(8,),
        in_specs=[packed(), pairs(), pairs(), pairs(), MAP, MAP, TAB],
        out_specs=pairs(),
        out_shape=GRID,
        compiler_params=params(32),
        name="last",
    )(arr, current, speed_ratio, pressure, zmap, vmap0, tab)
    return (final, current)


def solution(mesh):
    torus = Mesh(
        mesh.devices.reshape(4, 4, 2, mesh.shape["pen"]), ("slab_0", "slab_1", "slab_2", "pen")
    )
    placed = (
        P(SLAB, "pen", None),
        P(SLAB, "pen", None),
        P(SLAB, "pen", None),
        P(None, SLAB_PEN),
        P(),
        P(),
    )
    return jax.shard_map(
        step_pair,
        mesh=torus,
        in_specs=placed,
        out_specs=(P(SLAB, "pen", None), P(SLAB, "pen", None)),
        check_vma=False,
    )
```

```python
import math

import jax
import jax.numpy as jnp
import numpy as np
from jax import lax
from jax.experimental import pallas as pl
from jax.experimental.pallas import tpu as pltpu
from jax.sharding import Mesh
from jax.sharding import PartitionSpec as P

NX = 512
NY = 512
NZ = 512
HALF = 256
SENSORS = 2048
SLAB = ("slab_0", "slab_1", "slab_2")
SLAB_PEN = ("slab_0", "slab_1", "slab_2", "pen")
HALF_CFL = 0.25
MIB = 1024 * 1024
F32 = jnp.float32
BF16 = jnp.bfloat16


def half_tables():
    m = np.arange(HALF)[:, None]
    n = np.arange(HALF)[None, :]
    parts = []
    for freq in (2 * m, 2 * m + 1):
        angle = (freq * n % 512) * (2.0 * math.pi / 512)
        parts.append(np.cos(angle) + np.sin(angle))
    even, odd = parts
    stack = []
    for table in (even, odd, odd.T):
        high = table.astype(BF16)
        low = (table - high.astype(np.float64)).astype(BF16)
        stack += [high, low]
    return np.stack(stack)


EVEN, ODD, ODD_T = 0, 2, 4


def split(x):
    high = x.astype(BF16)
    low = (x - high.astype(F32)).astype(BF16)
    return high, low


def split3(x, axis):
    high, low = split(x)
    return jnp.concatenate([high, low, high], axis=axis)


def table3(tab, which, axis):
    high = tab[which]
    return jnp.concatenate([high, high, tab[which + 1]], axis=axis)


def dot(left, right, dims):
    return lax.dot_general(left, right, (dims, ((), ())), preferred_element_type=F32)


def cell_kernel(offs, vox, zmap):
    z = vox[0:1, :] - offs[0]
    y = vox[1:2, :] - offs[1]
    inside = (z >= 0) & (z < 16) & (y >= 0) & (y < 128)
    y = jnp.where(inside, y, -1)
    rows128 = lax.broadcasted_iota(jnp.int32, (128, SENSORS), 0)
    lhs = jnp.where(rows128 == y, (z + 1).astype(F32), 0.0).astype(BF16)
    columns = lax.broadcasted_iota(jnp.int32, (NX, SENSORS), 0)
    oncol = (columns == vox[2:3, :]).astype(F32).astype(BF16)
    zmap[...] = dot(lhs, oncol, ((1,), (1,))).astype(jnp.int32) - 1


def value_kernel(offs, vox, tcol, gathered, vmap0, vmap1, row0):
    z = vox[0:1, :] - offs[0]
    y = vox[1:2, :] - offs[1]
    tile = tcol[...] // 16
    lane = tcol[...] % 16
    inside = (z >= 0) & (z < 16) & (y >= 0) & (y < 128)
    y = jnp.where(inside, y, -1)
    rows128 = lax.broadcasted_iota(jnp.int32, (128, SENSORS), 0)
    pick = (rows128 == tile).astype(F32).astype(BF16)
    g = gathered[...].T
    g0, g1 = split(g)
    g2 = (g - g0.astype(F32) - g1.astype(F32)).astype(BF16)
    parts = dot(jnp.concatenate([g0, g1, g2], axis=0), pick, ((1,), (0,)))
    spread = parts[0:32] + parts[32:64] + parts[64:96]
    rows16 = lax.broadcasted_iota(jnp.int32, (16, SENSORS), 0)
    here = rows16 == lane
    onrow = rows128 == y
    lhs = []
    for t in range(2):
        value = jnp.sum(jnp.where(here, spread[16 * t : 16 * t + 16], 0.0), axis=0, keepdims=True)
        if t == 0:
            row0[...] = value
        v0 = value.astype(BF16).astype(F32)
        v1 = (value - v0).astype(BF16).astype(F32)
        v2 = value - v0 - v1
        for part in (v0, v1, v2):
            lhs.append(jnp.where(onrow, part, 0.0).astype(BF16))
    columns = lax.broadcasted_iota(jnp.int32, (NX, SENSORS), 0)
    oncol = (columns == vox[2:3, :]).astype(F32).astype(BF16)
    out = dot(jnp.concatenate(lhs, axis=0), oncol, ((1,), (1,)))
    vmap0[...] = out[0:128] + out[128:256] + out[256:384]
    vmap1[...] = out[384:512] + out[512:640] + out[640:768]


def seed_kernel(vox, weight, out):
    rows = lax.broadcasted_iota(jnp.int32, (512, SENSORS), 0)
    onrow = rows == vox[0:1, :]
    oncol = (rows == vox[1:2, :]).astype(F32).astype(BF16)
    value = weight[pl.ds(pl.program_id(0), 1), :]
    high = value.astype(BF16).astype(F32)
    low = value - high
    lhs = [jnp.where(onrow, part, 0.0).astype(BF16) for part in (high, low)]
    got = dot(jnp.concatenate(lhs, axis=0), oncol, ((1,), (1,)))
    out[0] = got[:512] + got[512:]


def forward_x(cur, tab, out):
    flat = cur.reshape(256, NX)
    a, b = flat[:, :HALF], flat[:, HALF:]
    out2 = out.reshape(1024, 128)
    for part, (which, data) in enumerate(((EVEN, a + b), (ODD, a - b))):
        got = dot(table3(tab, which, 1), split3(data, 1), ((1,), (1,)))
        for k in range(2):
            for z in range(2):
                out2[pl.ds(z * 4 + part * 2 + k, 128, stride=8), :] = got[
                    k * 128 : (k + 1) * 128, z * 128 : (z + 1) * 128
                ]


def inverse_x(arr, tab):
    arr2 = arr.reshape(1024, 128)
    halves = []
    for part, which in enumerate((EVEN, ODD)):
        pieces = []
        for z in range(2):
            rows = [arr2[pl.ds(z * 4 + part * 2 + k, 128, stride=8), :] for k in range(2)]
            pieces.append(jnp.concatenate(rows, axis=0))
        data = jnp.concatenate(pieces, axis=1)
        halves.append(dot(split3(data, 0), table3(tab, which, 0), ((0,), (0,))))
    even, odd = halves
    return jnp.concatenate([even + odd, even - odd], axis=1).reshape(2, 128, NX)


def inject(base, zmap, vmap):
    z = lax.broadcasted_iota(jnp.int32, (2, 1, 1), 0) + 2 * pl.program_id(0)
    return jnp.where(zmap[...][None] == z, vmap[...][None], base)


def first_kernel(p, zmap, tab, out):
    z = lax.broadcasted_iota(jnp.int32, (2, 1, 1), 0) + 2 * pl.program_id(0)
    forward_x(jnp.where(zmap[...][None] == z, 0.0, p[...]), tab, out)


def middle_kernel(arr, prev, speed, p, zmap, vmap0, vmap1, tab, cur_out, out):
    update = inverse_x(arr, tab)
    now = inject(p[...], zmap, vmap0)
    following = 2.0 * now - prev[...] + speed[...] * update
    cur = inject(following, zmap, vmap1)
    cur_out[...] = cur
    forward_x(cur, tab, out)


def last_kernel(arr, cur, speed, p, zmap, vmap0, tab, final):
    update = inverse_x(arr, tab)
    before = inject(p[...], zmap, vmap0)
    final[...] = 2.0 * cur[...] - before + speed[...] * update


def seeded_kernel(arr, seed, sym, tab, out):
    spectral_kernel(arr, sym, tab, out, seed)


def spectral_kernel(arr, sym, tab, out, seed=None):
    k = pl.program_id(0)
    pens = [arr[:, p, pl.ds(k, 16, stride=4), :].reshape(512, 128) for p in range(4)]
    a = jnp.concatenate(pens[:2], axis=1)
    b = jnp.concatenate(pens[2:], axis=1)
    if seed is not None:
        a = a + seed[0, :, :HALF]
        b = b + seed[0, :, HALF:]
    back = []
    for part, data in enumerate((a + b, a - b)):
        which = (EVEN, ODD_T)[part]
        x = dot(split3(data, 1), table3(tab, which, 0), ((1,), (0,)))
        top, bottom = x[:HALF], x[HALF:]
        even = dot(table3(tab, EVEN, 1), split3(top + bottom, 0), ((1,), (0,)))
        odd = dot(table3(tab, ODD, 1), split3(top - bottom, 0), ((1,), (0,)))
        cols = pl.ds(part * HALF, HALF)
        even = even * sym[0, pl.ds(0, HALF), cols]
        odd = odd * sym[0, pl.ds(HALF, HALF), cols]
        even = dot(table3(tab, EVEN, 1), split3(even, 0), ((1,), (0,)))
        odd = dot(table3(tab, ODD_T, 1), split3(odd, 0), ((1,), (0,)))
        z = jnp.concatenate([even + odd, even - odd], axis=0)
        back.append(dot(split3(z, 1), table3(tab, (EVEN, ODD)[part], 0), ((1,), (0,))))
    a = back[0] + back[1]
    b = back[0] - back[1]
    for p in range(4):
        piece = (a, b)[p // 2][:, (p % 2) * 128 : (p % 2) * 128 + 128]
        out[:, p, pl.ds(k, 16, stride=4), :] = piece.reshape(32, 16, 128)


def whole(*shape):
    return pl.BlockSpec(shape, lambda i: (0,) * len(shape))


def pairs():
    return pl.BlockSpec((2, 128, NX), lambda i: (i, 0, 0))


def packed():
    return pl.BlockSpec((128, 8, 128), lambda i: (0, i, 0))


def params(mib):
    return pltpu.CompilerParams(vmem_limit_bytes=mib * MIB)


TAB = whole(6, HALF, HALF)
MAP = whole(128, NX)
GRID = jax.ShapeDtypeStruct((16, 128, NX), F32)
WIRE = jax.ShapeDtypeStruct((128, 64, 128), F32)


def squared_freq(indices, length):
    signed_index = jnp.where(2 * indices > length, indices - length, indices)
    angular = signed_index.astype(F32) * (2.0 * math.pi / length)
    return angular * angular


def half_order(rows):
    return jnp.where(rows < HALF, 2 * rows, 2 * (rows - HALF) + 1)


def local_freq(device):
    return half_order(jnp.arange(4, dtype=jnp.int32) * 128 + device)


def symbol_of(device):
    rows = jnp.arange(512, dtype=jnp.int32)
    freq = squared_freq(half_order(rows), 512)
    freq_x = squared_freq(local_freq(device), NX)
    total = freq[None, :, None] + freq[None, None, :] + freq_x[:, None, None]
    square = total * (HALF_CFL * HALF_CFL)
    ratio = jnp.full_like(square, 1.0 / math.factorial(15) * -1.0)
    for n in (13, 11, 9, 7, 5, 3, 1):
        sign = 1.0 if n % 4 == 1 else -1.0
        ratio = ratio * square + sign / math.factorial(n)
    scale = -4.0 / (NX * NY * NZ)
    return square * ratio * ratio * scale


def exchange(array):
    return lax.all_to_all(array, SLAB_PEN, split_axis=0, concat_axis=0, tiled=True)


def step_pair(pressure, previous, speed_ratio, traces, sensor_voxels, trace_column):
    slab_index = lax.axis_index(SLAB)
    pen_index = lax.axis_index("pen")
    device = slab_index * 4 + pen_index
    tab = jnp.asarray(half_tables())
    offs = jnp.stack([slab_index * 16, pen_index * 128]).astype(jnp.int32)
    in_smem = pl.BlockSpec(memory_space=pltpu.SMEM)
    in_vmem = pl.BlockSpec(memory_space=pltpu.VMEM)
    gathered = exchange(jnp.broadcast_to(traces.reshape(1, 1, 32), (128, 1, 32)))
    zmap = pl.pallas_call(
        cell_kernel,
        in_specs=[in_smem, in_vmem],
        out_specs=in_vmem,
        out_shape=jax.ShapeDtypeStruct((128, NX), jnp.int32),
        compiler_params=params(8),
        name="cells",
    )(offs, sensor_voxels)
    wire = pl.pallas_call(
        first_kernel,
        grid=(8,),
        in_specs=[pairs(), MAP, TAB],
        out_specs=packed(),
        out_shape=pltpu.HBM((128, 64, 128), F32),
        compiler_params=params(12),
        name="first",
    )(pressure, zmap, tab)
    arr = exchange(wire)

    map_type = jax.ShapeDtypeStruct((128, NX), F32)
    vmap0, vmap1, row0 = pl.pallas_call(
        value_kernel,
        in_specs=[in_smem] + [in_vmem] * 3,
        out_specs=(in_vmem,) * 3,
        out_shape=(map_type, map_type, jax.ShapeDtypeStruct((1, SENSORS), F32)),
        compiler_params=params(16),
        name="values",
    )(offs, sensor_voxels, trace_column.reshape(1, SENSORS), gathered.reshape(128, 32))
    angle = (local_freq(device)[:, None] * sensor_voxels[2][None, :] % NX).astype(F32) * (2.0 * math.pi / NX)
    weight = row0 * (jnp.cos(angle) + jnp.sin(angle))
    plane = pl.BlockSpec((1, 512, 512), lambda i: (i, 0, 0))
    seed = pl.pallas_call(
        seed_kernel,
        grid=(4,),
        in_specs=[whole(3, SENSORS), whole(4, SENSORS)],
        out_specs=plane,
        out_shape=pltpu.HBM((4, 512, 512), F32),
        compiler_params=params(12),
        name="seeds",
    )(sensor_voxels, weight)
    sym = symbol_of(device)

    def spectral(arr, *extra):
        symbol = pltpu.with_memory_space_constraint(sym, pltpu.HBM) if extra else sym
        return pl.pallas_call(
            seeded_kernel if extra else spectral_kernel,
            grid=(4,),
            in_specs=[whole(32, 4, 64, 128)] + [plane] * (len(extra) + 1) + [TAB],
            out_specs=whole(32, 4, 64, 128),
            out_shape=jax.ShapeDtypeStruct((32, 4, 64, 128), F32),
            compiler_params=params(24),
            name="seeded" if extra else "spectral",
        )(arr.reshape(32, 4, 64, 128), *extra, symbol, tab).reshape(128, 64, 128)

    arr = exchange(spectral(arr, pltpu.with_memory_space_constraint(seed, pltpu.HBM)))
    current, wire = pl.pallas_call(
        middle_kernel,
        grid=(8,),
        in_specs=[packed(), pairs(), pairs(), pairs(), MAP, MAP, MAP, TAB],
        out_specs=(pairs(), packed()),
        out_shape=(GRID, WIRE),
        compiler_params=params(16),
        name="middle",
    )(arr, previous, speed_ratio, pressure, zmap, vmap0, vmap1, tab)
    arr = exchange(spectral(exchange(wire)))
    final = pl.pallas_call(
        last_kernel,
        grid=(8,),
        in_specs=[packed(), pairs(), pairs(), pairs(), MAP, MAP, TAB],
        out_specs=pairs(),
        out_shape=GRID,
        compiler_params=params(16),
        name="last",
    )(arr, current, speed_ratio, pressure, zmap, vmap0, tab)
    return (final, current)


def solution(mesh):
    torus = Mesh(
        mesh.devices.reshape(4, 4, 2, mesh.shape["pen"]), ("slab_0", "slab_1", "slab_2", "pen")
    )
    placed = (
        P(SLAB, "pen", None),
        P(SLAB, "pen", None),
        P(SLAB, "pen", None),
        P(None, SLAB_PEN),
        P(),
        P(),
    )
    return jax.shard_map(
        step_pair,
        mesh=torus,
        in_specs=placed,
        out_specs=(P(SLAB, "pen", None), P(SLAB, "pen", None)),
        check_vma=False,
    )
```

```python
import math

import jax
import jax.numpy as jnp
import numpy as np
from jax import lax
from jax.experimental import pallas as pl
from jax.experimental.pallas import tpu as pltpu
from jax.sharding import Mesh
from jax.sharding import PartitionSpec as P

NX = 512
NY = 512
NZ = 512
HALF = 256
SENSORS = 2048
SLAB = ("slab_0", "slab_1", "slab_2")
SLAB_PEN = ("slab_0", "slab_1", "slab_2", "pen")
HALF_CFL = 0.25
MIB = 1024 * 1024
ZB = 4
PZ = 2
F32 = jnp.float32
BF16 = jnp.bfloat16


def half_tables():
    m = np.arange(HALF)[:, None]
    n = np.arange(HALF)[None, :]
    parts = []
    for freq in (2 * m, 2 * m + 1):
        angle = (freq * n % 512) * (2.0 * math.pi / 512)
        parts.append(np.cos(angle) + np.sin(angle))
    even, odd = parts
    stack = []
    for table in (even, odd, odd.T):
        high = table.astype(BF16)
        low = (table - high.astype(np.float64)).astype(BF16)
        stack += [high, low]
    return np.stack(stack)


EVEN, ODD, ODD_T = 0, 2, 4


def split(x):
    high = x.astype(BF16)
    low = (x - high.astype(F32)).astype(BF16)
    return high, low


def split3(x, axis):
    high, low = split(x)
    return jnp.concatenate([high, low, high], axis=axis)


def table3(tab, which, axis):
    high = tab[which]
    return jnp.concatenate([high, high, tab[which + 1]], axis=axis)


def dot(left, right, dims):
    return lax.dot_general(left, right, (dims, ((), ())), preferred_element_type=F32)


def cell_kernel(offs, vox, zmap):
    z = vox[0:1, :] - offs[0]
    y = vox[1:2, :] - offs[1]
    inside = (z >= 0) & (z < 16) & (y >= 0) & (y < 128)
    y = jnp.where(inside, y, -1)
    rows128 = lax.broadcasted_iota(jnp.int32, (128, SENSORS), 0)
    lhs = jnp.where(rows128 == y, (z + 1).astype(F32), 0.0).astype(BF16)
    columns = lax.broadcasted_iota(jnp.int32, (NX, SENSORS), 0)
    oncol = (columns == vox[2:3, :]).astype(F32).astype(BF16)
    zmap[...] = dot(lhs, oncol, ((1,), (1,))).astype(jnp.int32) - 1


def value_kernel(offs, vox, tcol, gathered, vmap0, vmap1, row0):
    z = vox[0:1, :] - offs[0]
    y = vox[1:2, :] - offs[1]
    tile = tcol[...] // 16
    lane = tcol[...] % 16
    inside = (z >= 0) & (z < 16) & (y >= 0) & (y < 128)
    y = jnp.where(inside, y, -1)
    rows128 = lax.broadcasted_iota(jnp.int32, (128, SENSORS), 0)
    pick = (rows128 == tile).astype(F32).astype(BF16)
    g = gathered[...].T
    g0, g1 = split(g)
    g2 = (g - g0.astype(F32) - g1.astype(F32)).astype(BF16)
    parts = dot(jnp.concatenate([g0, g1, g2], axis=0), pick, ((1,), (0,)))
    spread = parts[0:32] + parts[32:64] + parts[64:96]
    rows16 = lax.broadcasted_iota(jnp.int32, (16, SENSORS), 0)
    here = rows16 == lane
    onrow = rows128 == y
    lhs = []
    for t in range(2):
        value = jnp.sum(jnp.where(here, spread[16 * t : 16 * t + 16], 0.0), axis=0, keepdims=True)
        if t == 0:
            row0[...] = value
        v0 = value.astype(BF16).astype(F32)
        v1 = (value - v0).astype(BF16).astype(F32)
        v2 = value - v0 - v1
        for part in (v0, v1, v2):
            lhs.append(jnp.where(onrow, part, 0.0).astype(BF16))
    columns = lax.broadcasted_iota(jnp.int32, (NX, SENSORS), 0)
    oncol = (columns == vox[2:3, :]).astype(F32).astype(BF16)
    out = dot(jnp.concatenate(lhs, axis=0), oncol, ((1,), (1,)))
    vmap0[...] = out[0:128] + out[128:256] + out[256:384]
    vmap1[...] = out[384:512] + out[512:640] + out[640:768]


def seed_kernel(vox, weight, out):
    rows = lax.broadcasted_iota(jnp.int32, (512, SENSORS), 0)
    onrow = rows == vox[0:1, :]
    oncol = (rows == vox[1:2, :]).astype(F32).astype(BF16)
    value = weight[pl.ds(pl.program_id(0), 1), :]
    high = value.astype(BF16).astype(F32)
    low = value - high
    lhs = [jnp.where(onrow, part, 0.0).astype(BF16) for part in (high, low)]
    got = dot(jnp.concatenate(lhs, axis=0), oncol, ((1,), (1,)))
    out[0] = got[:512] + got[512:]


def forward_x(cur, tab, out):
    sums = []
    for piece in cur:
        flat = piece.reshape(PZ * 128, NX)
        sums.append((flat[:, :HALF] + flat[:, HALF:], flat[:, :HALF] - flat[:, HALF:]))
    got = [
        [dot(table3(tab, (EVEN, ODD)[part], 1), split3(pair[part], 1), ((1,), (1,))) for part in range(2)]
        for pair in sums
    ]
    for i, pair in enumerate(got):
        for part in range(2):
            pieces = [pair[part][:, z * 128 : (z + 1) * 128].reshape(64, 4, 128) for z in range(2)]
            out[pl.ds(part * 64, 64), pl.ds(i * 8, 8), :] = jnp.concatenate(pieces, axis=1)


def inverse_x(arr, tab):
    halves = []
    for i in range(ZB // PZ):
        parts = []
        for part, which in enumerate((EVEN, ODD)):
            block = arr[pl.ds(part * 64, 64), pl.ds(i * 8, 8), :]
            pieces = [block[:, z * 4 : z * 4 + 4].reshape(HALF, 128) for z in range(2)]
            data = jnp.concatenate(pieces, axis=1)
            parts.append(dot(split3(data.T, 1), table3(tab, which, 0), ((1,), (0,))))
        halves.append(parts)
    return [
        jnp.concatenate([even + odd, even - odd], axis=1).reshape(PZ, 128, NX) for even, odd in halves
    ]


def planes(i):
    return pl.ds(i * PZ, PZ)


def here(zmap, i):
    z = lax.broadcasted_iota(jnp.int32, (PZ, 1, 1), 0) + ZB * pl.program_id(0) + i * PZ
    return zmap[...][None] == z


def first_kernel(p, zmap, tab, out):
    forward_x([jnp.where(here(zmap, i), 0.0, p[planes(i)]) for i in range(ZB // PZ)], tab, out)


def middle_kernel(arr, prev, speed, p, zmap, vmap0, vmap1, tab, cur_out, out):
    current = []
    for i, update in enumerate(inverse_x(arr, tab)):
        hit = here(zmap, i)
        now = jnp.where(hit, vmap0[...][None], p[planes(i)])
        following = 2.0 * now - prev[planes(i)] + speed[planes(i)] * update
        cur = jnp.where(hit, vmap1[...][None], following)
        cur_out[planes(i)] = cur
        current.append(cur)
    forward_x(current, tab, out)


def last_kernel(arr, cur, speed, p, zmap, vmap0, tab, final):
    for i, update in enumerate(inverse_x(arr, tab)):
        before = jnp.where(here(zmap, i), vmap0[...][None], p[planes(i)])
        final[planes(i)] = 2.0 * cur[planes(i)] - before + speed[planes(i)] * update


def seeded_kernel(arr, seed, sym, tab, out):
    spectral_kernel(arr, sym, tab, out, seed)


def spectral_kernel(arr, sym, tab, out, seed=None):
    step = pl.program_id(0)
    by_y = []
    for j in range(2):
        k = step * 2 + j
        pens = [arr[:, p, pl.ds(k, 16, stride=4), :].reshape(512, 128) for p in range(4)]
        a = jnp.concatenate(pens[:2], axis=1)
        b = jnp.concatenate(pens[2:], axis=1)
        if seed is not None:
            a = a + seed[j, :, :HALF]
            b = b + seed[j, :, HALF:]
        by_y += [
            dot(split3(data, 1), table3(tab, which, 0), ((1,), (0,)))
            for which, data in ((EVEN, a + b), (ODD_T, a - b))
        ]
    by_z = []
    for x in by_y:
        top, bottom = x[:HALF], x[HALF:]
        by_z.append(dot(table3(tab, EVEN, 1), split3(top + bottom, 0), ((1,), (0,))))
        by_z.append(dot(table3(tab, ODD, 1), split3(top - bottom, 0), ((1,), (0,))))
    scaled = [
        x * sym[i // 4, pl.ds(i % 2 * HALF, HALF), pl.ds(i % 4 // 2 * HALF, HALF)] for i, x in enumerate(by_z)
    ]
    back_z = [
        dot(table3(tab, (EVEN, ODD_T)[i % 2], 1), split3(x, 0), ((1,), (0,)))
        for i, x in enumerate(scaled)
    ]
    back_y = []
    for part in range(4):
        even, odd = back_z[2 * part], back_z[2 * part + 1]
        z = jnp.concatenate([even + odd, even - odd], axis=0)
        back_y.append(dot(split3(z, 1), table3(tab, (EVEN, ODD)[part % 2], 0), ((1,), (0,))))
    for j in range(2):
        a = back_y[2 * j] + back_y[2 * j + 1]
        b = back_y[2 * j] - back_y[2 * j + 1]
        for p in range(4):
            piece = (a, b)[p // 2][:, (p % 2) * 128 : (p % 2) * 128 + 128]
            out[:, p, pl.ds(step * 2 + j, 16, stride=4), :] = piece.reshape(32, 16, 128)


def whole(*shape):
    return pl.BlockSpec(shape, lambda i: (0,) * len(shape))


def pairs():
    return pl.BlockSpec((ZB, 128, NX), lambda i: (i, 0, 0))


def packed():
    return pl.BlockSpec((128, 4 * ZB, 128), lambda i: (0, i, 0))


def params(mib):
    return pltpu.CompilerParams(vmem_limit_bytes=mib * MIB)


TAB = whole(6, HALF, HALF)
MAP = whole(128, NX)
GRID = jax.ShapeDtypeStruct((16, 128, NX), F32)
WIRE = jax.ShapeDtypeStruct((128, 64, 128), F32)


def squared_freq(indices, length):
    signed_index = jnp.where(2 * indices > length, indices - length, indices)
    angular = signed_index.astype(F32) * (2.0 * math.pi / length)
    return angular * angular


def half_order(rows):
    return jnp.where(rows < HALF, 2 * rows, 2 * (rows - HALF) + 1)


def local_freq(device):
    return half_order(device * 4 + jnp.arange(4, dtype=jnp.int32))


def symbol_of(device):
    rows = jnp.arange(512, dtype=jnp.int32)
    freq = squared_freq(half_order(rows), 512)
    freq_x = squared_freq(local_freq(device), NX)
    total = freq[None, :, None] + freq[None, None, :] + freq_x[:, None, None]
    square = total * (HALF_CFL * HALF_CFL)
    ratio = jnp.full_like(square, 1.0 / math.factorial(15) * -1.0)
    for n in (13, 11, 9, 7, 5, 3, 1):
        sign = 1.0 if n % 4 == 1 else -1.0
        ratio = ratio * square + sign / math.factorial(n)
    scale = -4.0 / (NX * NY * NZ)
    return square * ratio * ratio * scale


def exchange(array):
    return lax.all_to_all(array, SLAB_PEN, split_axis=0, concat_axis=0, tiled=True)


def step_pair(pressure, previous, speed_ratio, traces, sensor_voxels, trace_column):
    slab_index = lax.axis_index(SLAB)
    pen_index = lax.axis_index("pen")
    device = slab_index * 4 + pen_index
    tab = jnp.asarray(half_tables())
    offs = jnp.stack([slab_index * 16, pen_index * 128]).astype(jnp.int32)
    in_smem = pl.BlockSpec(memory_space=pltpu.SMEM)
    in_vmem = pl.BlockSpec(memory_space=pltpu.VMEM)
    gathered = exchange(jnp.broadcast_to(traces.reshape(1, 1, 32), (128, 1, 32)))
    zmap = pl.pallas_call(
        cell_kernel,
        in_specs=[in_smem, in_vmem],
        out_specs=in_vmem,
        out_shape=jax.ShapeDtypeStruct((128, NX), jnp.int32),
        compiler_params=params(8),
        name="cells",
    )(offs, sensor_voxels)
    wire = pl.pallas_call(
        first_kernel,
        grid=(16 // ZB,),
        in_specs=[pairs(), MAP, TAB],
        out_specs=packed(),
        out_shape=pltpu.HBM((128, 64, 128), F32),
        compiler_params=params(16),
        name="first",
    )(pressure, zmap, tab)
    arr = exchange(wire)

    map_type = jax.ShapeDtypeStruct((128, NX), F32)
    vmap0, vmap1, row0 = pl.pallas_call(
        value_kernel,
        in_specs=[in_smem] + [in_vmem] * 3,
        out_specs=(in_vmem,) * 3,
        out_shape=(map_type, map_type, jax.ShapeDtypeStruct((1, SENSORS), F32)),
        compiler_params=params(16),
        name="values",
    )(offs, sensor_voxels, trace_column.reshape(1, SENSORS), gathered.reshape(128, 32))
    angle = (local_freq(device)[:, None] * sensor_voxels[2][None, :] % NX).astype(F32) * (2.0 * math.pi / NX)
    weight = row0 * (jnp.cos(angle) + jnp.sin(angle))
    plane = pl.BlockSpec((1, 512, 512), lambda i: (i, 0, 0))
    planes2 = pl.BlockSpec((2, 512, 512), lambda i: (i, 0, 0))
    seed = pl.pallas_call(
        seed_kernel,
        grid=(4,),
        in_specs=[whole(3, SENSORS), whole(4, SENSORS)],
        out_specs=plane,
        out_shape=pltpu.HBM((4, 512, 512), F32),
        compiler_params=params(12),
        name="seeds",
    )(sensor_voxels, weight)
    sym = symbol_of(device)

    def spectral(arr, *extra):
        symbol = pltpu.with_memory_space_constraint(sym, pltpu.HBM) if extra else sym
        return pl.pallas_call(
            seeded_kernel if extra else spectral_kernel,
            grid=(2,),
            in_specs=[whole(32, 4, 64, 128)] + [planes2] * (len(extra) + 1) + [TAB],
            out_specs=whole(32, 4, 64, 128),
            out_shape=jax.ShapeDtypeStruct((32, 4, 64, 128), F32),
            compiler_params=params(32),
            name="seeded" if extra else "spectral",
        )(arr.reshape(32, 4, 64, 128), *extra, symbol, tab).reshape(128, 64, 128)

    arr = exchange(spectral(arr, pltpu.with_memory_space_constraint(seed, pltpu.HBM)))
    current, wire = pl.pallas_call(
        middle_kernel,
        grid=(16 // ZB,),
        in_specs=[packed(), pairs(), pairs(), pairs(), MAP, MAP, MAP, TAB],
        out_specs=(pairs(), packed()),
        out_shape=(GRID, WIRE),
        compiler_params=params(24),
        name="middle",
    )(arr, previous, speed_ratio, pressure, zmap, vmap0, vmap1, tab)
    arr = exchange(spectral(exchange(wire)))
    final = pl.pallas_call(
        last_kernel,
        grid=(16 // ZB,),
        in_specs=[packed(), pairs(), pairs(), pairs(), MAP, MAP, TAB],
        out_specs=pairs(),
        out_shape=GRID,
        compiler_params=params(24),
        name="last",
    )(arr, current, speed_ratio, pressure, zmap, vmap0, tab)
    return (final, current)


def solution(mesh):
    torus = Mesh(
        mesh.devices.reshape(4, 4, 2, mesh.shape["pen"]), ("slab_0", "slab_1", "slab_2", "pen")
    )
    placed = (
        P(SLAB, "pen", None),
        P(SLAB, "pen", None),
        P(SLAB, "pen", None),
        P(None, SLAB_PEN),
        P(),
        P(),
    )
    return jax.shard_map(
        step_pair,
        mesh=torus,
        in_specs=placed,
        out_specs=(P(SLAB, "pen", None), P(SLAB, "pen", None)),
        check_vma=False,
    )
```

```python
import math

import jax
import jax.numpy as jnp
import numpy as np
from jax import lax
from jax.experimental import pallas as pl
from jax.experimental.pallas import tpu as pltpu
from jax.sharding import Mesh
from jax.sharding import PartitionSpec as P

NX = 512
NY = 512
NZ = 512
HALF = 256
SENSORS = 2048
SLAB = ("slab_0", "slab_1", "slab_2")
SLAB_PEN = ("slab_0", "slab_1", "slab_2", "pen")
HALF_CFL = 0.25
MIB = 1024 * 1024
ZB = 4
PZ = 2
F32 = jnp.float32
BF16 = jnp.bfloat16


def half_tables():
    m = np.arange(HALF)[:, None]
    n = np.arange(HALF)[None, :]
    parts = []
    for freq in (2 * m, 2 * m + 1):
        angle = (freq * n % 512) * (2.0 * math.pi / 512)
        parts.append(np.cos(angle) + np.sin(angle))
    even, odd = parts
    stack = []
    for table in (even, odd, odd.T):
        high = table.astype(BF16)
        low = (table - high.astype(np.float64)).astype(BF16)
        stack += [high, low]
    return np.stack(stack)


EVEN, ODD, ODD_T = 0, 2, 4


def split(x):
    high = x.astype(BF16)
    low = (x - high.astype(F32)).astype(BF16)
    return high, low


def split3(x, axis):
    high, low = split(x)
    return jnp.concatenate([high, low, high], axis=axis)


def table3(tab, which, axis):
    high = tab[which]
    return jnp.concatenate([high, high, tab[which + 1]], axis=axis)


def dot(left, right, dims):
    return lax.dot_general(left, right, (dims, ((), ())), preferred_element_type=F32)


def cell_kernel(offs, vox, traces, zmap, spread):
    spread[...] = jnp.broadcast_to(traces[...][None], (128, 2, 16))
    z = vox[0:1, :] - offs[0]
    y = vox[1:2, :] - offs[1]
    inside = (z >= 0) & (z < 16) & (y >= 0) & (y < 128)
    y = jnp.where(inside, y, -1)
    rows128 = lax.broadcasted_iota(jnp.int32, (128, SENSORS), 0)
    lhs = jnp.where(rows128 == y, (z + 1).astype(F32), 0.0).astype(BF16)
    columns = lax.broadcasted_iota(jnp.int32, (NX, SENSORS), 0)
    oncol = (columns == vox[2:3, :]).astype(F32).astype(BF16)
    zmap[...] = dot(lhs, oncol, ((1,), (1,))).astype(jnp.int32) - 1


def value_kernel(offs, vox, tcol, gathered, vmap0, vmap1, row0):
    z = vox[0:1, :] - offs[0]
    y = vox[1:2, :] - offs[1]
    tile = tcol[...] // 16
    lane = tcol[...] % 16
    inside = (z >= 0) & (z < 16) & (y >= 0) & (y < 128)
    y = jnp.where(inside, y, -1)
    rows128 = lax.broadcasted_iota(jnp.int32, (128, SENSORS), 0)
    pick = (rows128 == tile).astype(F32).astype(BF16)
    g = gathered[...].T
    g0, g1 = split(g)
    g2 = (g - g0.astype(F32) - g1.astype(F32)).astype(BF16)
    parts = dot(jnp.concatenate([g0, g1, g2], axis=0), pick, ((1,), (0,)))
    spread = parts[0:32] + parts[32:64] + parts[64:96]
    rows16 = lax.broadcasted_iota(jnp.int32, (16, SENSORS), 0)
    here = rows16 == lane
    onrow = rows128 == y
    lhs = []
    for t in range(2):
        value = jnp.sum(jnp.where(here, spread[16 * t : 16 * t + 16], 0.0), axis=0, keepdims=True)
        if t == 0:
            row0[...] = value
        v0 = value.astype(BF16).astype(F32)
        v1 = (value - v0).astype(BF16).astype(F32)
        v2 = value - v0 - v1
        for part in (v0, v1, v2):
            lhs.append(jnp.where(onrow, part, 0.0).astype(BF16))
    columns = lax.broadcasted_iota(jnp.int32, (NX, SENSORS), 0)
    oncol = (columns == vox[2:3, :]).astype(F32).astype(BF16)
    out = dot(jnp.concatenate(lhs, axis=0), oncol, ((1,), (1,)))
    vmap0[...] = out[0:128] + out[128:256] + out[256:384]
    vmap1[...] = out[384:512] + out[512:640] + out[640:768]


def to_y(a, b, tab):
    return [
        dot(split3(data, 1), table3(tab, which, 0), ((1,), (0,)))
        for which, data in ((EVEN, a + b), (ODD_T, a - b))
    ]


def to_z(by_y, tab):
    by_z = []
    for x in by_y:
        top, bottom = x[:HALF], x[HALF:]
        by_z.append(dot(table3(tab, EVEN, 1), split3(top + bottom, 0), ((1,), (0,))))
        by_z.append(dot(table3(tab, ODD, 1), split3(top - bottom, 0), ((1,), (0,))))
    return by_z


def quarter(i):
    return pl.ds(i % 2 * HALF, HALF), pl.ds(i // 2 * HALF, HALF)


def seed_kernel(vox, weight, tab, out):
    rows = lax.broadcasted_iota(jnp.int32, (512, SENSORS), 0)
    onrow = rows == vox[0:1, :]
    oncol = (rows == vox[1:2, :]).astype(F32).astype(BF16)
    value = weight[pl.ds(pl.program_id(0), 1), :]
    high = value.astype(BF16).astype(F32)
    low = value - high
    lhs = [jnp.where(onrow, part, 0.0).astype(BF16) for part in (high, low)]
    got = dot(jnp.concatenate(lhs, axis=0), oncol, ((1,), (1,)))
    got = got[:512] + got[512:]
    for i, x in enumerate(to_z(to_y(got[:, :HALF], got[:, HALF:], tab), tab)):
        rows_of, cols_of = quarter(i)
        out[0, rows_of, cols_of] = x


def forward_x(cur, tab, out):
    sums = []
    for piece in cur:
        flat = piece.reshape(PZ * 128, NX)
        sums.append((flat[:, :HALF] + flat[:, HALF:], flat[:, :HALF] - flat[:, HALF:]))
    got = [
        [dot(table3(tab, (EVEN, ODD)[part], 1), split3(pair[part], 1), ((1,), (1,))) for part in range(2)]
        for pair in sums
    ]
    for i, pair in enumerate(got):
        for part in range(2):
            pieces = [pair[part][:, z * 128 : (z + 1) * 128].reshape(64, 4, 128) for z in range(2)]
            out[pl.ds(part * 64, 64), pl.ds(i * 8, 8), :] = jnp.concatenate(pieces, axis=1)


def inverse_x(arr, tab):
    halves = []
    for i in range(ZB // PZ):
        parts = []
        for part, which in enumerate((EVEN, ODD)):
            block = arr[pl.ds(part * 64, 64), pl.ds(i * 8, 8), :]
            pieces = [block[:, z * 4 : z * 4 + 4].reshape(HALF, 128) for z in range(2)]
            data = jnp.concatenate(pieces, axis=1)
            parts.append(dot(split3(data.T, 1), table3(tab, which, 0), ((1,), (0,))))
        halves.append(parts)
    return [
        jnp.concatenate([even + odd, even - odd], axis=1).reshape(PZ, 128, NX) for even, odd in halves
    ]


def planes(i):
    return pl.ds(i * PZ, PZ)


def here(zmap, i):
    z = lax.broadcasted_iota(jnp.int32, (PZ, 1, 1), 0) + ZB * pl.program_id(0) + i * PZ
    return zmap[...][None] == z


def first_kernel(p, zmap, tab, out):
    forward_x([jnp.where(here(zmap, i), 0.0, p[planes(i)]) for i in range(ZB // PZ)], tab, out)


def middle_kernel(arr, prev, speed, p, zmap, vmap0, vmap1, tab, cur_out, out):
    current = []
    for i, update in enumerate(inverse_x(arr, tab)):
        hit = here(zmap, i)
        now = jnp.where(hit, vmap0[...][None], p[planes(i)])
        following = 2.0 * now - prev[planes(i)] + speed[planes(i)] * update
        cur = jnp.where(hit, vmap1[...][None], following)
        cur_out[planes(i)] = cur
        current.append(cur)
    forward_x(current, tab, out)


def last_kernel(arr, cur, speed, p, zmap, vmap0, tab, final):
    for i, update in enumerate(inverse_x(arr, tab)):
        before = jnp.where(here(zmap, i), vmap0[...][None], p[planes(i)])
        final[planes(i)] = 2.0 * cur[planes(i)] - before + speed[planes(i)] * update


def seeded_kernel(arr, seed, sym, tab, out, seed_v, sym_v, sems):
    step = pl.program_id(0)

    def copy(which, h):
        src, dst = ((seed, seed_v), (sym, sym_v))[which]
        planes_of = pl.ds(2 * h, 2)
        return pltpu.make_async_copy(src.at[planes_of], dst.at[planes_of], sems.at[which, h])

    @pl.when(step == 0)
    def _():
        for h in range(2):
            copy(0, h).start()
            copy(1, h).start()

    by_z = analyse(arr, tab, step)
    copy(0, step).wait()
    copy(1, step).wait()
    for j in range(2):
        for i in range(4):
            rows_of, cols_of = quarter(i)
            k = 2 * step + j
            by_z[4 * j + i] = (by_z[4 * j + i] + seed_v[k, rows_of, cols_of]) * sym_v[k, rows_of, cols_of]
    synthesise(by_z, tab, out, step)


def spectral_kernel(arr, sym, tab, out):
    step = pl.program_id(0)
    by_z = analyse(arr, tab, step)
    for j in range(2):
        for i in range(4):
            rows_of, cols_of = quarter(i)
            by_z[4 * j + i] = by_z[4 * j + i] * sym[j, rows_of, cols_of]
    synthesise(by_z, tab, out, step)


def analyse(arr, tab, step):
    by_y = []
    for j in range(2):
        k = step * 2 + j
        pens = [arr[:, p, pl.ds(k, 16, stride=4), :].reshape(512, 128) for p in range(4)]
        by_y += to_y(jnp.concatenate(pens[:2], axis=1), jnp.concatenate(pens[2:], axis=1), tab)
    return to_z(by_y, tab)


def synthesise(scaled, tab, out, step):
    back_z = [
        dot(table3(tab, (EVEN, ODD_T)[i % 2], 1), split3(x, 0), ((1,), (0,)))
        for i, x in enumerate(scaled)
    ]
    back_y = []
    for part in range(4):
        even, odd = back_z[2 * part], back_z[2 * part + 1]
        z = jnp.concatenate([even + odd, even - odd], axis=0)
        back_y.append(dot(split3(z, 1), table3(tab, (EVEN, ODD)[part % 2], 0), ((1,), (0,))))
    for j in range(2):
        a = back_y[2 * j] + back_y[2 * j + 1]
        b = back_y[2 * j] - back_y[2 * j + 1]
        for p in range(4):
            piece = (a, b)[p // 2][:, (p % 2) * 128 : (p % 2) * 128 + 128]
            out[:, p, pl.ds(step * 2 + j, 16, stride=4), :] = piece.reshape(32, 16, 128)


def whole(*shape):
    return pl.BlockSpec(shape, lambda i: (0,) * len(shape))


def pairs():
    return pl.BlockSpec((ZB, 128, NX), lambda i: (i, 0, 0))


def packed():
    return pl.BlockSpec((128, 4 * ZB, 128), lambda i: (0, i, 0))


def params(mib):
    return pltpu.CompilerParams(vmem_limit_bytes=mib * MIB)


TAB = whole(6, HALF, HALF)
MAP = whole(128, NX)
GRID = jax.ShapeDtypeStruct((16, 128, NX), F32)
WIRE = jax.ShapeDtypeStruct((128, 64, 128), F32)


def squared_freq(indices, length):
    signed_index = jnp.where(2 * indices > length, indices - length, indices)
    angular = signed_index.astype(F32) * (2.0 * math.pi / length)
    return angular * angular


def half_order(rows):
    return jnp.where(rows < HALF, 2 * rows, 2 * (rows - HALF) + 1)


def local_freq(device):
    return half_order(device * 4 + jnp.arange(4, dtype=jnp.int32))


def symbol_of(device):
    rows = jnp.arange(512, dtype=jnp.int32)
    freq = squared_freq(half_order(rows), 512)
    freq_x = squared_freq(local_freq(device), NX)
    total = freq[None, :, None] + freq[None, None, :] + freq_x[:, None, None]
    square = total * (HALF_CFL * HALF_CFL)
    ratio = jnp.full_like(square, 1.0 / math.factorial(15) * -1.0)
    for n in (13, 11, 9, 7, 5, 3, 1):
        sign = 1.0 if n % 4 == 1 else -1.0
        ratio = ratio * square + sign / math.factorial(n)
    scale = -4.0 / (NX * NY * NZ)
    return square * ratio * ratio * scale


def in_hbm(array):
    return pltpu.with_memory_space_constraint(array, pltpu.HBM)


def exchange(array):
    return lax.all_to_all(array, SLAB_PEN, split_axis=0, concat_axis=0, tiled=True)


def step_pair(pressure, previous, speed_ratio, traces, sensor_voxels, trace_column):
    slab_index = lax.axis_index(SLAB)
    pen_index = lax.axis_index("pen")
    device = slab_index * 4 + pen_index
    tab = jnp.asarray(half_tables())
    offs = jnp.stack([slab_index * 16, pen_index * 128]).astype(jnp.int32)
    in_smem = pl.BlockSpec(memory_space=pltpu.SMEM)
    in_vmem = pl.BlockSpec(memory_space=pltpu.VMEM)
    zmap, copies = pl.pallas_call(
        cell_kernel,
        in_specs=[in_smem, in_vmem, in_vmem],
        out_specs=(in_vmem, in_vmem),
        out_shape=(
            jax.ShapeDtypeStruct((128, NX), jnp.int32),
            jax.ShapeDtypeStruct((128, 2, 16), F32),
        ),
        compiler_params=params(8),
        name="cells",
    )(offs, sensor_voxels, traces)
    gathered = exchange(copies)
    wire = pl.pallas_call(
        first_kernel,
        grid=(16 // ZB,),
        in_specs=[pairs(), MAP, TAB],
        out_specs=packed(),
        out_shape=pltpu.HBM((128, 64, 128), F32),
        compiler_params=params(16),
        name="first",
    )(in_hbm(pressure), zmap, in_hbm(tab))
    arr = exchange(wire)

    map_type = jax.ShapeDtypeStruct((128, NX), F32)
    vmap0, vmap1, row0 = pl.pallas_call(
        value_kernel,
        in_specs=[in_smem] + [in_vmem] * 3,
        out_specs=(in_vmem,) * 3,
        out_shape=(map_type, map_type, jax.ShapeDtypeStruct((1, SENSORS), F32)),
        compiler_params=params(16),
        name="values",
    )(offs, sensor_voxels, trace_column.reshape(1, SENSORS), gathered.reshape(128, 32))
    angle = (local_freq(device)[:, None] * sensor_voxels[2][None, :] % NX).astype(F32) * (2.0 * math.pi / NX)
    weight = row0 * (jnp.cos(angle) + jnp.sin(angle))
    plane = pl.BlockSpec((1, 512, 512), lambda i: (i, 0, 0))
    planes2 = pl.BlockSpec((2, 512, 512), lambda i: (i, 0, 0))
    seed = pl.pallas_call(
        seed_kernel,
        grid=(4,),
        in_specs=[whole(3, SENSORS), whole(4, SENSORS), TAB],
        out_specs=plane,
        out_shape=pltpu.HBM((4, 512, 512), F32),
        compiler_params=params(12),
        name="seeds",
    )(sensor_voxels, weight, tab)
    sym = symbol_of(device)

    cube = whole(32, 4, 64, 128)
    cube_type = jax.ShapeDtypeStruct((32, 4, 64, 128), F32)
    raw = pl.BlockSpec(memory_space=pl.ANY)
    arr = pl.pallas_call(
        seeded_kernel,
        grid=(2,),
        in_specs=[cube, raw, raw, TAB],
        out_specs=cube,
        out_shape=cube_type,
        scratch_shapes=[
            pltpu.VMEM((4, 512, 512), F32),
            pltpu.VMEM((4, 512, 512), F32),
            pltpu.SemaphoreType.DMA((2, 2)),
        ],
        compiler_params=params(32),
        name="seeded",
    )(arr.reshape(32, 4, 64, 128), in_hbm(seed), in_hbm(sym), tab)
    arr = exchange(arr.reshape(128, 64, 128))
    current, wire = pl.pallas_call(
        middle_kernel,
        grid=(16 // ZB,),
        in_specs=[packed(), pairs(), pairs(), pairs(), MAP, MAP, MAP, TAB],
        out_specs=(pairs(), packed()),
        out_shape=(GRID, WIRE),
        compiler_params=params(24),
        name="middle",
    )(arr, previous, speed_ratio, pressure, zmap, vmap0, vmap1, tab)
    arr = pl.pallas_call(
        spectral_kernel,
        grid=(2,),
        in_specs=[cube, planes2, TAB],
        out_specs=cube,
        out_shape=cube_type,
        compiler_params=params(24),
        name="spectral",
    )(exchange(wire).reshape(32, 4, 64, 128), sym, tab)
    arr = exchange(arr.reshape(128, 64, 128))
    final = pl.pallas_call(
        last_kernel,
        grid=(16 // ZB,),
        in_specs=[packed(), pairs(), pairs(), pairs(), MAP, MAP, TAB],
        out_specs=pairs(),
        out_shape=GRID,
        compiler_params=params(24),
        name="last",
    )(arr, current, speed_ratio, pressure, zmap, vmap0, tab)
    return (final, current)


def solution(mesh):
    torus = Mesh(
        mesh.devices.reshape(4, 4, 2, mesh.shape["pen"]), ("slab_0", "slab_1", "slab_2", "pen")
    )
    placed = (
        P(SLAB, "pen", None),
        P(SLAB, "pen", None),
        P(SLAB, "pen", None),
        P(None, SLAB_PEN),
        P(),
        P(),
    )
    return jax.shard_map(
        step_pair,
        mesh=torus,
        in_specs=placed,
        out_specs=(P(SLAB, "pen", None), P(SLAB, "pen", None)),
        check_vma=False,
    )
```

```python
import math

import jax
import jax.numpy as jnp
import numpy as np
from jax import lax
from jax.experimental import pallas as pl
from jax.experimental.pallas import tpu as pltpu
from jax.sharding import Mesh
from jax.sharding import PartitionSpec as P

NX = 512
NY = 512
NZ = 512
HALF = 256
SENSORS = 2048
SLAB = ("slab_0", "slab_1", "slab_2")
SLAB_PEN = ("slab_0", "slab_1", "slab_2", "pen")
HALF_CFL = 0.25
MIB = 1024 * 1024
ZB = 4
PZ = 2
F32 = jnp.float32
BF16 = jnp.bfloat16


def half_tables():
    m = np.arange(HALF)[:, None]
    n = np.arange(HALF)[None, :]
    parts = []
    for freq in (2 * m, 2 * m + 1):
        angle = (freq * n % 512) * (2.0 * math.pi / 512)
        parts.append(np.cos(angle) + np.sin(angle))
    even, odd = parts
    stack = []
    for table in (even, odd, odd.T):
        high = table.astype(BF16)
        low = (table - high.astype(np.float64)).astype(BF16)
        stack += [high, low]
    return np.stack(stack)


EVEN, ODD, ODD_T = 0, 2, 4


def split(x):
    high = x.astype(BF16)
    low = (x - high.astype(F32)).astype(BF16)
    return high, low


def split3(x, axis):
    high, low = split(x)
    return jnp.concatenate([high, low, high], axis=axis)


def table3(tab, which, axis):
    high = tab[which]
    return jnp.concatenate([high, high, tab[which + 1]], axis=axis)


def dot(left, right, dims):
    return lax.dot_general(left, right, (dims, ((), ())), preferred_element_type=F32)


def fill_maps(offs, vox, tcol, gathered, zmap, vmap0, vmap1):
    z = vox[0:1, :] - offs[0]
    y = vox[1:2, :] - offs[1]
    tile = tcol[...] // 16
    lane = tcol[...] % 16
    inside = (z >= 0) & (z < 16) & (y >= 0) & (y < 128)
    y = jnp.where(inside, y, -1)
    rows128 = lax.broadcasted_iota(jnp.int32, (128, SENSORS), 0)
    pick = (rows128 == tile).astype(F32).astype(BF16)
    g = gathered[...].T
    g0, g1 = split(g)
    g2 = (g - g0.astype(F32) - g1.astype(F32)).astype(BF16)
    parts = dot(jnp.concatenate([g0, g1, g2], axis=0), pick, ((1,), (0,)))
    spread = parts[0:32] + parts[32:64] + parts[64:96]
    rows16 = lax.broadcasted_iota(jnp.int32, (16, SENSORS), 0)
    here = rows16 == lane
    onrow = rows128 == y
    lhs = [jnp.where(onrow, (z + 1).astype(F32), 0.0).astype(BF16)]
    for t in range(2):
        value = jnp.sum(jnp.where(here, spread[16 * t : 16 * t + 16], 0.0), axis=0, keepdims=True)
        v0 = value.astype(BF16).astype(F32)
        v1 = (value - v0).astype(BF16).astype(F32)
        v2 = value - v0 - v1
        for part in (v0, v1, v2):
            lhs.append(jnp.where(onrow, part, 0.0).astype(BF16))
    columns = lax.broadcasted_iota(jnp.int32, (NX, SENSORS), 0)
    oncol = (columns == vox[2:3, :]).astype(F32).astype(BF16)
    out = dot(jnp.concatenate(lhs, axis=0), oncol, ((1,), (1,)))
    zmap[...] = out[0:128].astype(jnp.int32) - 1
    vmap0[...] = out[128:256] + out[256:384] + out[384:512]
    vmap1[...] = out[512:640] + out[640:768] + out[768:896]


def to_y(a, b, tab):
    return [
        dot(split3(data, 1), table3(tab, which, 0), ((1,), (0,)))
        for which, data in ((EVEN, a + b), (ODD_T, a - b))
    ]


def to_z(by_y, tab):
    by_z = []
    for x in by_y:
        top, bottom = x[:HALF], x[HALF:]
        by_z.append(dot(table3(tab, EVEN, 1), split3(top + bottom, 0), ((1,), (0,))))
        by_z.append(dot(table3(tab, ODD, 1), split3(top - bottom, 0), ((1,), (0,))))
    return by_z


def quarter(i):
    return pl.ds(i % 2 * HALF, HALF), pl.ds(i // 2 * HALF, HALF)


def forward_x(cur, tab, out):
    sums = []
    for piece in cur:
        flat = piece.reshape(PZ * 128, NX)
        sums.append((flat[:, :HALF] + flat[:, HALF:], flat[:, :HALF] - flat[:, HALF:]))
    got = [
        [dot(table3(tab, (EVEN, ODD)[part], 1), split3(pair[part], 1), ((1,), (1,))) for part in range(2)]
        for pair in sums
    ]
    for i, pair in enumerate(got):
        for part in range(2):
            pieces = [pair[part][:, z * 128 : (z + 1) * 128].reshape(64, 4, 128) for z in range(2)]
            out[pl.ds(part * 64, 64), pl.ds(i * 8, 8), :] = jnp.concatenate(pieces, axis=1)


def inverse_x(arr, tab):
    halves = []
    for i in range(ZB // PZ):
        parts = []
        for part, which in enumerate((EVEN, ODD)):
            block = arr[pl.ds(part * 64, 64), pl.ds(i * 8, 8), :]
            pieces = [block[:, z * 4 : z * 4 + 4].reshape(HALF, 128) for z in range(2)]
            data = jnp.concatenate(pieces, axis=1)
            parts.append(dot(split3(data.T, 1), table3(tab, which, 0), ((1,), (0,))))
        halves.append(parts)
    return [
        jnp.concatenate([even + odd, even - odd], axis=1).reshape(PZ, 128, NX) for even, odd in halves
    ]


def planes(i):
    return pl.ds(i * PZ, PZ)


def here(zmap, i):
    z = lax.broadcasted_iota(jnp.int32, (PZ, 1, 1), 0) + ZB * pl.program_id(0) + i * PZ
    return zmap[...][None] == z


def first_kernel(offs, vox, tcol, gathered, p, tab, zmap, vmap0, vmap1, out):
    @pl.when(pl.program_id(0) == 0)
    def _():
        fill_maps(offs, vox, tcol, gathered, zmap, vmap0, vmap1)

    forward_x(
        [jnp.where(here(zmap, i), vmap0[...][None], p[planes(i)]) for i in range(ZB // PZ)], tab, out
    )


def middle_kernel(arr, prev, speed, p, zmap, vmap0, vmap1, tab, cur_out, out):
    current = []
    for i, update in enumerate(inverse_x(arr, tab)):
        hit = here(zmap, i)
        now = jnp.where(hit, vmap0[...][None], p[planes(i)])
        following = 2.0 * now - prev[planes(i)] + speed[planes(i)] * update
        cur = jnp.where(hit, vmap1[...][None], following)
        cur_out[planes(i)] = cur
        current.append(cur)
    forward_x(current, tab, out)


def last_kernel(arr, cur, speed, p, zmap, vmap0, tab, final):
    for i, update in enumerate(inverse_x(arr, tab)):
        before = jnp.where(here(zmap, i), vmap0[...][None], p[planes(i)])
        final[planes(i)] = 2.0 * cur[planes(i)] - before + speed[planes(i)] * update


def spectral_kernel(arr, sym, tab, out):
    step = pl.program_id(0)
    by_z = analyse(arr, tab, step)
    for j in range(2):
        for i in range(4):
            rows_of, cols_of = quarter(i)
            by_z[4 * j + i] = by_z[4 * j + i] * sym[j, rows_of, cols_of]
    synthesise(by_z, tab, out, step)


def analyse(arr, tab, step):
    by_y = []
    for j in range(2):
        k = step * 2 + j
        pens = [arr[:, p, pl.ds(k, 16, stride=4), :].reshape(512, 128) for p in range(4)]
        by_y += to_y(jnp.concatenate(pens[:2], axis=1), jnp.concatenate(pens[2:], axis=1), tab)
    return to_z(by_y, tab)


def synthesise(scaled, tab, out, step):
    back_z = [
        dot(table3(tab, (EVEN, ODD_T)[i % 2], 1), split3(x, 0), ((1,), (0,)))
        for i, x in enumerate(scaled)
    ]
    back_y = []
    for part in range(4):
        even, odd = back_z[2 * part], back_z[2 * part + 1]
        z = jnp.concatenate([even + odd, even - odd], axis=0)
        back_y.append(dot(split3(z, 1), table3(tab, (EVEN, ODD)[part % 2], 0), ((1,), (0,))))
    for j in range(2):
        a = back_y[2 * j] + back_y[2 * j + 1]
        b = back_y[2 * j] - back_y[2 * j + 1]
        for p in range(4):
            piece = (a, b)[p // 2][:, (p % 2) * 128 : (p % 2) * 128 + 128]
            out[:, p, pl.ds(step * 2 + j, 16, stride=4), :] = piece.reshape(32, 16, 128)


def whole(*shape):
    return pl.BlockSpec(shape, lambda i: (0,) * len(shape))


def pairs():
    return pl.BlockSpec((ZB, 128, NX), lambda i: (i, 0, 0))


def packed():
    return pl.BlockSpec((128, 4 * ZB, 128), lambda i: (0, i, 0))


def params(mib):
    return pltpu.CompilerParams(vmem_limit_bytes=mib * MIB)


TAB = whole(6, HALF, HALF)
MAP = whole(128, NX)
GRID = jax.ShapeDtypeStruct((16, 128, NX), F32)
WIRE = jax.ShapeDtypeStruct((128, 64, 128), F32)


def squared_freq(indices, length):
    signed_index = jnp.where(2 * indices > length, indices - length, indices)
    angular = signed_index.astype(F32) * (2.0 * math.pi / length)
    return angular * angular


def half_order(rows):
    return jnp.where(rows < HALF, 2 * rows, 2 * (rows - HALF) + 1)


def local_freq(device):
    return half_order(device * 4 + jnp.arange(4, dtype=jnp.int32))


def symbol_of(device):
    rows = jnp.arange(512, dtype=jnp.int32)
    freq = squared_freq(half_order(rows), 512)
    freq_x = squared_freq(local_freq(device), NX)
    total = freq[None, :, None] + freq[None, None, :] + freq_x[:, None, None]
    square = total * (HALF_CFL * HALF_CFL)
    ratio = jnp.full_like(square, 1.0 / math.factorial(15) * -1.0)
    for n in (13, 11, 9, 7, 5, 3, 1):
        sign = 1.0 if n % 4 == 1 else -1.0
        ratio = ratio * square + sign / math.factorial(n)
    scale = -4.0 / (NX * NY * NZ)
    return square * ratio * ratio * scale


def in_hbm(array):
    return pltpu.with_memory_space_constraint(array, pltpu.HBM)


def exchange(array):
    return lax.all_to_all(array, SLAB_PEN, split_axis=0, concat_axis=0, tiled=True)


def step_pair(pressure, previous, speed_ratio, traces, sensor_voxels, trace_column):
    slab_index = lax.axis_index(SLAB)
    pen_index = lax.axis_index("pen")
    device = slab_index * 4 + pen_index
    tab = jnp.asarray(half_tables())
    offs = jnp.stack([slab_index * 16, pen_index * 128]).astype(jnp.int32)
    gathered = exchange(jnp.broadcast_to(traces[None], (128, 2, 16)))
    sym = symbol_of(device)
    in_smem = pl.BlockSpec(memory_space=pltpu.SMEM)
    map_type = jax.ShapeDtypeStruct((128, NX), F32)
    zmap, vmap0, vmap1, wire = pl.pallas_call(
        first_kernel,
        grid=(16 // ZB,),
        in_specs=[in_smem, whole(3, SENSORS), whole(1, SENSORS), whole(128, 32), pairs(), TAB],
        out_specs=(MAP, MAP, MAP, packed()),
        out_shape=(jax.ShapeDtypeStruct((128, NX), jnp.int32), map_type, map_type, WIRE),
        compiler_params=params(24),
        name="first",
    )(
        offs,
        sensor_voxels,
        trace_column.reshape(1, SENSORS),
        gathered.reshape(128, 32),
        in_hbm(pressure),
        tab,
    )
    cube = whole(32, 4, 64, 128)
    planes2 = pl.BlockSpec((2, 512, 512), lambda i: (i, 0, 0))

    def spectral(arr):
        return pl.pallas_call(
            spectral_kernel,
            grid=(2,),
            in_specs=[cube, planes2, TAB],
            out_specs=cube,
            out_shape=jax.ShapeDtypeStruct((32, 4, 64, 128), F32),
            compiler_params=params(24),
            name="spectral",
        )(arr.reshape(32, 4, 64, 128), sym, tab).reshape(128, 64, 128)

    arr = exchange(spectral(exchange(wire)))
    current, wire = pl.pallas_call(
        middle_kernel,
        grid=(16 // ZB,),
        in_specs=[packed(), pairs(), pairs(), pairs(), MAP, MAP, MAP, TAB],
        out_specs=(pairs(), packed()),
        out_shape=(GRID, WIRE),
        compiler_params=params(24),
        name="middle",
    )(arr, previous, speed_ratio, pressure, zmap, vmap0, vmap1, tab)
    arr = exchange(spectral(exchange(wire)))
    final = pl.pallas_call(
        last_kernel,
        grid=(16 // ZB,),
        in_specs=[packed(), pairs(), pairs(), pairs(), MAP, MAP, TAB],
        out_specs=pairs(),
        out_shape=GRID,
        compiler_params=params(24),
        name="last",
    )(arr, current, speed_ratio, pressure, zmap, vmap0, tab)
    return (final, current)


def solution(mesh):
    torus = Mesh(
        mesh.devices.reshape(4, 4, 2, mesh.shape["pen"]), ("slab_0", "slab_1", "slab_2", "pen")
    )
    placed = (
        P(SLAB, "pen", None),
        P(SLAB, "pen", None),
        P(SLAB, "pen", None),
        P(None, SLAB_PEN),
        P(),
        P(),
    )
    return jax.shard_map(
        step_pair,
        mesh=torus,
        in_specs=placed,
        out_specs=(P(SLAB, "pen", None), P(SLAB, "pen", None)),
        check_vma=False,
    )
```

```python
import math

import jax
import jax.numpy as jnp
import numpy as np
from jax import lax
from jax.experimental import pallas as pl
from jax.experimental.pallas import tpu as pltpu
from jax.sharding import Mesh
from jax.sharding import PartitionSpec as P

NX = 512
NY = 512
NZ = 512
HALF = 256
SENSORS = 2048
SLAB = ("slab_0", "slab_1", "slab_2")
SLAB_PEN = ("slab_0", "slab_1", "slab_2", "pen")
HALF_CFL = 0.25
MIB = 1024 * 1024
ZB = 4
PZ = 2
F32 = jnp.float32
BF16 = jnp.bfloat16


def half_tables():
    m = np.arange(HALF)[:, None]
    n = np.arange(HALF)[None, :]
    parts = []
    for freq in (2 * m, 2 * m + 1):
        angle = (freq * n % 512) * (2.0 * math.pi / 512)
        parts.append(np.cos(angle) + np.sin(angle))
    even, odd = parts
    stack = []
    for table in (even, odd, odd.T):
        high = table.astype(BF16)
        low = (table - high.astype(np.float64)).astype(BF16)
        stack += [high, low]
    return np.stack(stack)


EVEN, ODD, ODD_T = 0, 2, 4


def split(x):
    high = x.astype(BF16)
    low = (x - high.astype(F32)).astype(BF16)
    return high, low


def split3(x, axis):
    high, low = split(x)
    return jnp.concatenate([high, low, high], axis=axis)


def table3(tab, which, axis):
    high = tab[which]
    return jnp.concatenate([high, high, tab[which + 1]], axis=axis)


def dot(left, right, dims):
    return lax.dot_general(left, right, (dims, ((), ())), preferred_element_type=F32)


def fill_maps(offs, vox, tcol, gathered, zmap, vmap0, vmap1):
    z = vox[0:1, :] - offs[0]
    y = vox[1:2, :] - offs[1]
    tile = tcol[...] // 16
    lane = tcol[...] % 16
    inside = (z >= 0) & (z < 16) & (y >= 0) & (y < 128)
    y = jnp.where(inside, y, -1)
    rows128 = lax.broadcasted_iota(jnp.int32, (128, SENSORS), 0)
    pick = (rows128 == tile).astype(F32).astype(BF16)
    g = gathered[...].T
    g0, g1 = split(g)
    g2 = (g - g0.astype(F32) - g1.astype(F32)).astype(BF16)
    parts = dot(jnp.concatenate([g0, g1, g2], axis=0), pick, ((1,), (0,)))
    spread = parts[0:32] + parts[32:64] + parts[64:96]
    rows16 = lax.broadcasted_iota(jnp.int32, (16, SENSORS), 0)
    here = rows16 == lane
    onrow = rows128 == y
    lhs = [jnp.where(onrow, (z + 1).astype(F32), 0.0).astype(BF16)]
    for t in range(2):
        value = jnp.sum(jnp.where(here, spread[16 * t : 16 * t + 16], 0.0), axis=0, keepdims=True)
        v0 = value.astype(BF16).astype(F32)
        v1 = (value - v0).astype(BF16).astype(F32)
        v2 = value - v0 - v1
        for part in (v0, v1, v2):
            lhs.append(jnp.where(onrow, part, 0.0).astype(BF16))
    columns = lax.broadcasted_iota(jnp.int32, (NX, SENSORS), 0)
    oncol = (columns == vox[2:3, :]).astype(F32).astype(BF16)
    out = dot(jnp.concatenate(lhs, axis=0), oncol, ((1,), (1,)))
    zmap[...] = out[0:128].astype(jnp.int32) - 1
    vmap0[...] = out[128:256] + out[256:384] + out[384:512]
    vmap1[...] = out[512:640] + out[640:768] + out[768:896]


def to_y(a, b, tab):
    return [
        dot(split3(data, 1), table3(tab, which, 0), ((1,), (0,)))
        for which, data in ((EVEN, a + b), (ODD_T, a - b))
    ]


def to_z(by_y, tab):
    by_z = []
    for x in by_y:
        top, bottom = x[:HALF], x[HALF:]
        by_z.append(dot(table3(tab, EVEN, 1), split3(top + bottom, 0), ((1,), (0,))))
        by_z.append(dot(table3(tab, ODD, 1), split3(top - bottom, 0), ((1,), (0,))))
    return by_z


def quarter(i):
    return pl.ds(i % 2 * HALF, HALF), pl.ds(i // 2 * HALF, HALF)


def forward_x(cur, tab, out):
    sums = []
    for piece in cur:
        flat = piece.reshape(PZ * 128, NX)
        sums.append((flat[:, :HALF] + flat[:, HALF:], flat[:, :HALF] - flat[:, HALF:]))
    got = [
        [dot(table3(tab, (EVEN, ODD)[part], 1), split3(pair[part], 1), ((1,), (1,))) for part in range(2)]
        for pair in sums
    ]
    for i, pair in enumerate(got):
        for part in range(2):
            pieces = [pair[part][:, z * 128 : (z + 1) * 128].reshape(64, 4, 128) for z in range(2)]
            out[pl.ds(part * 64, 64), pl.ds(i * 8, 8), :] = jnp.concatenate(pieces, axis=1)


def inverse_x(arr, tab):
    halves = []
    for i in range(ZB // PZ):
        parts = []
        for part, which in enumerate((EVEN, ODD)):
            block = arr[pl.ds(part * 64, 64), pl.ds(i * 8, 8), :]
            pieces = [block[:, z * 4 : z * 4 + 4].reshape(HALF, 128) for z in range(2)]
            data = jnp.concatenate(pieces, axis=1)
            parts.append(dot(split3(data.T, 1), table3(tab, which, 0), ((1,), (0,))))
        halves.append(parts)
    return [
        jnp.concatenate([even + odd, even - odd], axis=1).reshape(PZ, 128, NX) for even, odd in halves
    ]


def planes(i):
    return pl.ds(i * PZ, PZ)


def here(zmap, i):
    z = lax.broadcasted_iota(jnp.int32, (PZ, 1, 1), 0) + ZB * pl.program_id(0) + i * PZ
    return zmap[...][None] == z


def first_kernel(offs, vox, tcol, gathered, p, tab, zmap, vmap0, vmap1, out, p_v, sems):
    step = pl.program_id(0)

    def copy(i):
        part = pl.ds(i * ZB, ZB)
        return pltpu.make_async_copy(p.at[part], p_v.at[part], sems.at[i])

    @pl.when(step == 0)
    def _():
        for i in range(16 // ZB):
            copy(i).start()
        fill_maps(offs, vox, tcol, gathered, zmap, vmap0, vmap1)

    copy(step).wait()
    base = step * ZB
    forward_x(
        [
            jnp.where(here(zmap, i), vmap0[...][None], p_v[pl.ds(base + i * PZ, PZ)])
            for i in range(ZB // PZ)
        ],
        tab,
        out,
    )


def middle_kernel(arr, prev, speed, p, zmap, vmap0, vmap1, tab, cur_out, out):
    current = []
    for i, update in enumerate(inverse_x(arr, tab)):
        hit = here(zmap, i)
        now = jnp.where(hit, vmap0[...][None], p[planes(i)])
        following = 2.0 * now - prev[planes(i)] + speed[planes(i)] * update
        cur = jnp.where(hit, vmap1[...][None], following)
        cur_out[planes(i)] = cur
        current.append(cur)
    forward_x(current, tab, out)


def last_kernel(arr, cur, speed, p, zmap, vmap0, tab, final):
    for i, update in enumerate(inverse_x(arr, tab)):
        before = jnp.where(here(zmap, i), vmap0[...][None], p[planes(i)])
        final[planes(i)] = 2.0 * cur[planes(i)] - before + speed[planes(i)] * update


def spectral_kernel(arr, sym, tab, out):
    step = pl.program_id(0)
    by_z = analyse(arr, tab, step)
    for j in range(2):
        for i in range(4):
            rows_of, cols_of = quarter(i)
            by_z[4 * j + i] = by_z[4 * j + i] * sym[j, rows_of, cols_of]
    synthesise(by_z, tab, out, step)


def analyse(arr, tab, step):
    by_y = []
    for j in range(2):
        k = step * 2 + j
        pens = [arr[:, p, pl.ds(k, 16, stride=4), :].reshape(512, 128) for p in range(4)]
        by_y += to_y(jnp.concatenate(pens[:2], axis=1), jnp.concatenate(pens[2:], axis=1), tab)
    return to_z(by_y, tab)


def synthesise(scaled, tab, out, step):
    back_z = [
        dot(table3(tab, (EVEN, ODD_T)[i % 2], 1), split3(x, 0), ((1,), (0,)))
        for i, x in enumerate(scaled)
    ]
    back_y = []
    for part in range(4):
        even, odd = back_z[2 * part], back_z[2 * part + 1]
        z = jnp.concatenate([even + odd, even - odd], axis=0)
        back_y.append(dot(split3(z, 1), table3(tab, (EVEN, ODD)[part % 2], 0), ((1,), (0,))))
    for j in range(2):
        a = back_y[2 * j] + back_y[2 * j + 1]
        b = back_y[2 * j] - back_y[2 * j + 1]
        for p in range(4):
            piece = (a, b)[p // 2][:, (p % 2) * 128 : (p % 2) * 128 + 128]
            out[:, p, pl.ds(step * 2 + j, 16, stride=4), :] = piece.reshape(32, 16, 128)


def whole(*shape):
    return pl.BlockSpec(shape, lambda i: (0,) * len(shape))


def pairs():
    return pl.BlockSpec((ZB, 128, NX), lambda i: (i, 0, 0))


def packed():
    return pl.BlockSpec((128, 4 * ZB, 128), lambda i: (0, i, 0))


def params(mib):
    return pltpu.CompilerParams(vmem_limit_bytes=mib * MIB)


TAB = whole(6, HALF, HALF)
MAP = whole(128, NX)
GRID = jax.ShapeDtypeStruct((16, 128, NX), F32)
WIRE = jax.ShapeDtypeStruct((128, 64, 128), F32)


def squared_freq(indices, length):
    signed_index = jnp.where(2 * indices > length, indices - length, indices)
    angular = signed_index.astype(F32) * (2.0 * math.pi / length)
    return angular * angular


def half_order(rows):
    return jnp.where(rows < HALF, 2 * rows, 2 * (rows - HALF) + 1)


def local_freq(device):
    return half_order(device * 4 + jnp.arange(4, dtype=jnp.int32))


def symbol_of(device):
    rows = jnp.arange(512, dtype=jnp.int32)
    freq = squared_freq(half_order(rows), 512)
    freq_x = squared_freq(local_freq(device), NX)
    total = freq[None, :, None] + freq[None, None, :] + freq_x[:, None, None]
    square = total * (HALF_CFL * HALF_CFL)
    ratio = jnp.full_like(square, 1.0 / math.factorial(15) * -1.0)
    for n in (13, 11, 9, 7, 5, 3, 1):
        sign = 1.0 if n % 4 == 1 else -1.0
        ratio = ratio * square + sign / math.factorial(n)
    scale = -4.0 / (NX * NY * NZ)
    return square * ratio * ratio * scale


def in_hbm(array):
    return pltpu.with_memory_space_constraint(array, pltpu.HBM)


def exchange(array):
    return lax.all_to_all(array, SLAB_PEN, split_axis=0, concat_axis=0, tiled=True)


def step_pair(pressure, previous, speed_ratio, traces, sensor_voxels, trace_column):
    slab_index = lax.axis_index(SLAB)
    pen_index = lax.axis_index("pen")
    device = slab_index * 4 + pen_index
    tab = jnp.asarray(half_tables())
    offs = jnp.stack([slab_index * 16, pen_index * 128]).astype(jnp.int32)
    gathered = exchange(jnp.broadcast_to(traces[None], (128, 2, 16)))
    sym = symbol_of(device)
    in_smem = pl.BlockSpec(memory_space=pltpu.SMEM)
    map_type = jax.ShapeDtypeStruct((128, NX), F32)
    zmap, vmap0, vmap1, wire = pl.pallas_call(
        first_kernel,
        grid=(16 // ZB,),
        in_specs=[in_smem, whole(3, SENSORS), whole(1, SENSORS), whole(128, 32), pl.BlockSpec(memory_space=pl.ANY), TAB],
        out_specs=(MAP, MAP, MAP, packed()),
        out_shape=(jax.ShapeDtypeStruct((128, NX), jnp.int32), map_type, map_type, WIRE),
        scratch_shapes=[pltpu.VMEM((16, 128, NX), F32), pltpu.SemaphoreType.DMA((16 // ZB,))],
        compiler_params=params(24),
        name="first",
    )(
        offs,
        sensor_voxels,
        trace_column.reshape(1, SENSORS),
        gathered.reshape(128, 32),
        in_hbm(pressure),
        tab,
    )
    cube = whole(32, 4, 64, 128)
    planes2 = pl.BlockSpec((2, 512, 512), lambda i: (i, 0, 0))

    def spectral(arr):
        return pl.pallas_call(
            spectral_kernel,
            grid=(2,),
            in_specs=[cube, planes2, TAB],
            out_specs=cube,
            out_shape=jax.ShapeDtypeStruct((32, 4, 64, 128), F32),
            compiler_params=params(24),
            name="spectral",
        )(arr.reshape(32, 4, 64, 128), sym, tab).reshape(128, 64, 128)

    arr = exchange(spectral(exchange(wire)))
    current, wire = pl.pallas_call(
        middle_kernel,
        grid=(16 // ZB,),
        in_specs=[packed(), pairs(), pairs(), pairs(), MAP, MAP, MAP, TAB],
        out_specs=(pairs(), packed()),
        out_shape=(GRID, WIRE),
        compiler_params=params(24),
        name="middle",
    )(arr, previous, speed_ratio, pressure, zmap, vmap0, vmap1, tab)
    arr = exchange(spectral(exchange(wire)))
    final = pl.pallas_call(
        last_kernel,
        grid=(16 // ZB,),
        in_specs=[packed(), pairs(), pairs(), pairs(), MAP, MAP, TAB],
        out_specs=pairs(),
        out_shape=GRID,
        compiler_params=params(24),
        name="last",
    )(arr, current, speed_ratio, pressure, zmap, vmap0, tab)
    return (final, current)


def solution(mesh):
    torus = Mesh(
        mesh.devices.reshape(4, 4, 2, mesh.shape["pen"]), ("slab_0", "slab_1", "slab_2", "pen")
    )
    placed = (
        P(SLAB, "pen", None),
        P(SLAB, "pen", None),
        P(SLAB, "pen", None),
        P(None, SLAB_PEN),
        P(),
        P(),
    )
    return jax.shard_map(
        step_pair,
        mesh=torus,
        in_specs=placed,
        out_specs=(P(SLAB, "pen", None), P(SLAB, "pen", None)),
        check_vma=False,
    )
```

```python
import math

import jax
import jax.numpy as jnp
import numpy as np
from jax import lax
from jax.experimental import pallas as pl
from jax.experimental.pallas import tpu as pltpu
from jax.sharding import Mesh
from jax.sharding import PartitionSpec as P

NX = 512
NY = 512
NZ = 512
HALF = 256
SENSORS = 2048
SLAB = ("slab_0", "slab_1", "slab_2")
SLAB_PEN = ("slab_0", "slab_1", "slab_2", "pen")
HALF_CFL = 0.25
MIB = 1024 * 1024
ZB = 16
PZ = 2
F32 = jnp.float32
BF16 = jnp.bfloat16


def half_tables():
    m = np.arange(HALF)[:, None]
    n = np.arange(HALF)[None, :]
    parts = []
    for freq in (2 * m, 2 * m + 1):
        angle = (freq * n % 512) * (2.0 * math.pi / 512)
        parts.append(np.cos(angle) + np.sin(angle))
    even, odd = parts
    stack = []
    for table in (even, odd, odd.T):
        high = table.astype(BF16)
        low = (table - high.astype(np.float64)).astype(BF16)
        stack += [high, low]
    return np.stack(stack)


EVEN, ODD, ODD_T = 0, 2, 4


def split(x):
    high = x.astype(BF16)
    low = (x - high.astype(F32)).astype(BF16)
    return high, low


def split3(x, axis):
    high, low = split(x)
    return jnp.concatenate([high, low, high], axis=axis)


def table3(tab, which, axis):
    high = tab[which]
    return jnp.concatenate([high, high, tab[which + 1]], axis=axis)


def dot(left, right, dims):
    return lax.dot_general(left, right, (dims, ((), ())), preferred_element_type=F32)


def fill_maps(offs, vox, tcol, gathered, zmap, vmap0, vmap1):
    z = vox[0:1, :] - offs[0]
    y = vox[1:2, :] - offs[1]
    tile = tcol[...] // 16
    lane = tcol[...] % 16
    inside = (z >= 0) & (z < 16) & (y >= 0) & (y < 128)
    y = jnp.where(inside, y, -1)
    rows128 = lax.broadcasted_iota(jnp.int32, (128, SENSORS), 0)
    pick = (rows128 == tile).astype(F32).astype(BF16)
    g = gathered[...].T
    g0, g1 = split(g)
    g2 = (g - g0.astype(F32) - g1.astype(F32)).astype(BF16)
    parts = dot(jnp.concatenate([g0, g1, g2], axis=0), pick, ((1,), (0,)))
    spread = parts[0:32] + parts[32:64] + parts[64:96]
    rows16 = lax.broadcasted_iota(jnp.int32, (16, SENSORS), 0)
    here = rows16 == lane
    onrow = rows128 == y
    lhs = [jnp.where(onrow, (z + 1).astype(F32), 0.0).astype(BF16)]
    for t in range(2):
        value = jnp.sum(jnp.where(here, spread[16 * t : 16 * t + 16], 0.0), axis=0, keepdims=True)
        v0 = value.astype(BF16).astype(F32)
        v1 = (value - v0).astype(BF16).astype(F32)
        v2 = value - v0 - v1
        for part in (v0, v1, v2):
            lhs.append(jnp.where(onrow, part, 0.0).astype(BF16))
    columns = lax.broadcasted_iota(jnp.int32, (NX, SENSORS), 0)
    oncol = (columns == vox[2:3, :]).astype(F32).astype(BF16)
    out = dot(jnp.concatenate(lhs, axis=0), oncol, ((1,), (1,)))
    zmap[...] = out[0:128].astype(jnp.int32) - 1
    vmap0[...] = out[128:256] + out[256:384] + out[384:512]
    vmap1[...] = out[512:640] + out[640:768] + out[768:896]


def to_y(a, b, tab):
    return [
        dot(split3(data, 1), table3(tab, which, 0), ((1,), (0,)))
        for which, data in ((EVEN, a + b), (ODD_T, a - b))
    ]


def to_z(by_y, tab):
    by_z = []
    for x in by_y:
        top, bottom = x[:HALF], x[HALF:]
        by_z.append(dot(table3(tab, EVEN, 1), split3(top + bottom, 0), ((1,), (0,))))
        by_z.append(dot(table3(tab, ODD, 1), split3(top - bottom, 0), ((1,), (0,))))
    return by_z


def quarter(i):
    return pl.ds(i % 2 * HALF, HALF), pl.ds(i // 2 * HALF, HALF)


def forward_x(cur, tab, out):
    sums = []
    for piece in cur:
        flat = piece.reshape(PZ * 128, NX)
        sums.append((flat[:, :HALF] + flat[:, HALF:], flat[:, :HALF] - flat[:, HALF:]))
    got = [
        [dot(table3(tab, (EVEN, ODD)[part], 1), split3(pair[part], 1), ((1,), (1,))) for part in range(2)]
        for pair in sums
    ]
    for i, pair in enumerate(got):
        for part in range(2):
            pieces = [pair[part][:, z * 128 : (z + 1) * 128].reshape(64, 4, 128) for z in range(2)]
            out[pl.ds(part * 64, 64), pl.ds(i * 8, 8), :] = jnp.concatenate(pieces, axis=1)


def inverse_x(arr, tab):
    halves = []
    for i in range(ZB // PZ):
        parts = []
        for part, which in enumerate((EVEN, ODD)):
            block = arr[pl.ds(part * 64, 64), pl.ds(i * 8, 8), :]
            pieces = [block[:, z * 4 : z * 4 + 4].reshape(HALF, 128) for z in range(2)]
            data = jnp.concatenate(pieces, axis=1)
            parts.append(dot(split3(data.T, 1), table3(tab, which, 0), ((1,), (0,))))
        halves.append(parts)
    return [
        jnp.concatenate([even + odd, even - odd], axis=1).reshape(PZ, 128, NX) for even, odd in halves
    ]


def planes(i):
    return pl.ds(i * PZ, PZ)


def here(zmap, i):
    z = lax.broadcasted_iota(jnp.int32, (PZ, 1, 1), 0) + ZB * pl.program_id(0) + i * PZ
    return zmap[...][None] == z


def first_kernel(offs, vox, tcol, gathered, p, tab, zmap, vmap0, vmap1, out, p_v, sems):
    step = pl.program_id(0)

    def copy(i):
        part = pl.ds(i * ZB, ZB)
        return pltpu.make_async_copy(p.at[part], p_v.at[part], sems.at[i])

    @pl.when(step == 0)
    def _():
        for i in range(16 // ZB):
            copy(i).start()
        fill_maps(offs, vox, tcol, gathered, zmap, vmap0, vmap1)

    copy(step).wait()
    base = step * ZB
    forward_x(
        [
            jnp.where(here(zmap, i), vmap0[...][None], p_v[pl.ds(base + i * PZ, PZ)])
            for i in range(ZB // PZ)
        ],
        tab,
        out,
    )


def write_back(scratch, target, sems, i):
    group = pl.program_id(0) * (ZB // PZ) + i
    part = pl.ds(group * PZ, PZ)
    return pltpu.make_async_copy(scratch.at[part], target.at[part], sems.at[group])


def wait_all(scratch, target, sems):
    @pl.when(pl.program_id(0) == 16 // ZB - 1)
    def _():
        for group in range(16 // PZ):
            part = pl.ds(group * PZ, PZ)
            pltpu.make_async_copy(scratch.at[part], target.at[part], sems.at[group]).wait()


def own_planes(i):
    return pl.ds(pl.program_id(0) * ZB + i * PZ, PZ)


def middle_kernel(arr, prev, speed, p, zmap, vmap0, vmap1, tab, cur_out, out, cur_v, sems):
    current = []
    for i, update in enumerate(inverse_x(arr, tab)):
        hit = here(zmap, i)
        now = jnp.where(hit, vmap0[...][None], p[planes(i)])
        following = 2.0 * now - prev[planes(i)] + speed[planes(i)] * update
        cur = jnp.where(hit, vmap1[...][None], following)
        cur_v[own_planes(i)] = cur
        write_back(cur_v, cur_out, sems, i).start()
        current.append(cur)
    forward_x(current, tab, out)
    wait_all(cur_v, cur_out, sems)


def last_kernel(arr, cur, speed, p, zmap, vmap0, tab, final, final_v, sems):
    for i, update in enumerate(inverse_x(arr, tab)):
        before = jnp.where(here(zmap, i), vmap0[...][None], p[planes(i)])
        final_v[own_planes(i)] = 2.0 * cur[planes(i)] - before + speed[planes(i)] * update
        write_back(final_v, final, sems, i).start()
    wait_all(final_v, final, sems)


def spectral_kernel(arr, sym, tab, out):
    step = pl.program_id(0)
    by_z = analyse(arr, tab, step)
    for j in range(2):
        for i in range(4):
            rows_of, cols_of = quarter(i)
            by_z[4 * j + i] = by_z[4 * j + i] * sym[j, rows_of, cols_of]
    synthesise(by_z, tab, out, step)


def analyse(arr, tab, step):
    by_y = []
    for j in range(2):
        k = step * 2 + j
        pens = [arr[:, p, pl.ds(k, 16, stride=4), :].reshape(512, 128) for p in range(4)]
        by_y += to_y(jnp.concatenate(pens[:2], axis=1), jnp.concatenate(pens[2:], axis=1), tab)
    return to_z(by_y, tab)


def synthesise(scaled, tab, out, step):
    back_z = [
        dot(table3(tab, (EVEN, ODD_T)[i % 2], 1), split3(x, 0), ((1,), (0,)))
        for i, x in enumerate(scaled)
    ]
    back_y = []
    for part in range(4):
        even, odd = back_z[2 * part], back_z[2 * part + 1]
        z = jnp.concatenate([even + odd, even - odd], axis=0)
        back_y.append(dot(split3(z, 1), table3(tab, (EVEN, ODD)[part % 2], 0), ((1,), (0,))))
    for j in range(2):
        a = back_y[2 * j] + back_y[2 * j + 1]
        b = back_y[2 * j] - back_y[2 * j + 1]
        for p in range(4):
            piece = (a, b)[p // 2][:, (p % 2) * 128 : (p % 2) * 128 + 128]
            out[:, p, pl.ds(step * 2 + j, 16, stride=4), :] = piece.reshape(32, 16, 128)


def whole(*shape):
    return pl.BlockSpec(shape, lambda i: (0,) * len(shape))


def pairs():
    return pl.BlockSpec((ZB, 128, NX), lambda i: (i, 0, 0))


def packed():
    return pl.BlockSpec((128, 4 * ZB, 128), lambda i: (0, i, 0))


def params(mib):
    return pltpu.CompilerParams(vmem_limit_bytes=mib * MIB)


TAB = whole(6, HALF, HALF)
MAP = whole(128, NX)
WIRE = jax.ShapeDtypeStruct((128, 64, 128), F32)


def squared_freq(indices, length):
    signed_index = jnp.where(2 * indices > length, indices - length, indices)
    angular = signed_index.astype(F32) * (2.0 * math.pi / length)
    return angular * angular


def half_order(rows):
    return jnp.where(rows < HALF, 2 * rows, 2 * (rows - HALF) + 1)


def local_freq(device):
    return half_order(device * 4 + jnp.arange(4, dtype=jnp.int32))


def symbol_of(device):
    rows = jnp.arange(512, dtype=jnp.int32)
    freq = squared_freq(half_order(rows), 512)
    freq_x = squared_freq(local_freq(device), NX)
    total = freq[None, :, None] + freq[None, None, :] + freq_x[:, None, None]
    square = total * (HALF_CFL * HALF_CFL)
    ratio = jnp.full_like(square, 1.0 / math.factorial(15) * -1.0)
    for n in (13, 11, 9, 7, 5, 3, 1):
        sign = 1.0 if n % 4 == 1 else -1.0
        ratio = ratio * square + sign / math.factorial(n)
    scale = -4.0 / (NX * NY * NZ)
    return square * ratio * ratio * scale


def in_hbm(array):
    return pltpu.with_memory_space_constraint(array, pltpu.HBM)


def exchange(array):
    return lax.all_to_all(array, SLAB_PEN, split_axis=0, concat_axis=0, tiled=True)


def step_pair(pressure, previous, speed_ratio, traces, sensor_voxels, trace_column):
    slab_index = lax.axis_index(SLAB)
    pen_index = lax.axis_index("pen")
    device = slab_index * 4 + pen_index
    tab = jnp.asarray(half_tables())
    offs = jnp.stack([slab_index * 16, pen_index * 128]).astype(jnp.int32)
    gathered = exchange(jnp.broadcast_to(traces[None], (128, 2, 16)))
    sym = symbol_of(device)
    in_smem = pl.BlockSpec(memory_space=pltpu.SMEM)
    map_type = jax.ShapeDtypeStruct((128, NX), F32)
    zmap, vmap0, vmap1, wire = pl.pallas_call(
        first_kernel,
        grid=(16 // ZB,),
        in_specs=[in_smem, whole(3, SENSORS), whole(1, SENSORS), whole(128, 32), pl.BlockSpec(memory_space=pl.ANY), TAB],
        out_specs=(MAP, MAP, MAP, packed()),
        out_shape=(jax.ShapeDtypeStruct((128, NX), jnp.int32), map_type, map_type, WIRE),
        scratch_shapes=[pltpu.VMEM((16, 128, NX), F32), pltpu.SemaphoreType.DMA((16 // ZB,))],
        compiler_params=params(24),
        name="first",
    )(
        offs,
        sensor_voxels,
        trace_column.reshape(1, SENSORS),
        gathered.reshape(128, 32),
        in_hbm(pressure),
        tab,
    )
    cube = whole(32, 4, 64, 128)
    planes2 = pl.BlockSpec((2, 512, 512), lambda i: (i, 0, 0))

    def spectral(arr):
        return pl.pallas_call(
            spectral_kernel,
            grid=(2,),
            in_specs=[cube, planes2, TAB],
            out_specs=cube,
            out_shape=jax.ShapeDtypeStruct((32, 4, 64, 128), F32),
            compiler_params=params(24),
            name="spectral",
        )(arr.reshape(32, 4, 64, 128), sym, tab).reshape(128, 64, 128)

    arr = exchange(spectral(exchange(wire)))
    current, wire = pl.pallas_call(
        middle_kernel,
        grid=(16 // ZB,),
        in_specs=[packed(), pairs(), pairs(), pairs(), MAP, MAP, MAP, TAB],
        out_specs=(pl.BlockSpec(memory_space=pl.ANY), packed()),
        out_shape=(pltpu.HBM((16, 128, NX), F32), WIRE),
        scratch_shapes=[pltpu.VMEM((16, 128, NX), F32), pltpu.SemaphoreType.DMA((16 // PZ,))],
        compiler_params=params(24),
        name="middle",
    )(arr, previous, speed_ratio, pressure, zmap, vmap0, vmap1, tab)
    arr = exchange(spectral(exchange(wire)))
    final = pl.pallas_call(
        last_kernel,
        grid=(16 // ZB,),
        in_specs=[packed(), pairs(), pairs(), pairs(), MAP, MAP, TAB],
        out_specs=pl.BlockSpec(memory_space=pl.ANY),
        out_shape=pltpu.HBM((16, 128, NX), F32),
        scratch_shapes=[pltpu.VMEM((16, 128, NX), F32), pltpu.SemaphoreType.DMA((16 // PZ,))],
        compiler_params=params(24),
        name="last",
    )(arr, current, speed_ratio, pressure, zmap, vmap0, tab)
    return (final, current)


def solution(mesh):
    torus = Mesh(
        mesh.devices.reshape(4, 4, 2, mesh.shape["pen"]), ("slab_0", "slab_1", "slab_2", "pen")
    )
    placed = (
        P(SLAB, "pen", None),
        P(SLAB, "pen", None),
        P(SLAB, "pen", None),
        P(None, SLAB_PEN),
        P(),
        P(),
    )
    return jax.shard_map(
        step_pair,
        mesh=torus,
        in_specs=placed,
        out_specs=(P(SLAB, "pen", None), P(SLAB, "pen", None)),
        check_vma=False,
    )
```

```python
import math

import jax
import jax.numpy as jnp
import numpy as np
from jax import lax
from jax.experimental import pallas as pl
from jax.experimental.pallas import tpu as pltpu
from jax.sharding import Mesh
from jax.sharding import PartitionSpec as P

NX = 512
NY = 512
NZ = 512
HALF = 256
SENSORS = 2048
SLAB = ("slab_0", "slab_1", "slab_2")
SLAB_PEN = ("slab_0", "slab_1", "slab_2", "pen")
HALF_CFL = 0.25
MIB = 1024 * 1024
ZB = 16
PZ = 2
F32 = jnp.float32
BF16 = jnp.bfloat16


def half_tables():
    m = np.arange(HALF)[:, None]
    n = np.arange(HALF)[None, :]
    parts = []
    for freq in (2 * m, 2 * m + 1):
        angle = (freq * n % 512) * (2.0 * math.pi / 512)
        parts.append(np.cos(angle) + np.sin(angle))
    even, odd = parts
    stack = []
    for table in (even, odd, odd.T):
        high = table.astype(BF16)
        low = (table - high.astype(np.float64)).astype(BF16)
        stack += [high, low]
    return np.stack(stack)


EVEN, ODD, ODD_T = 0, 2, 4


def split(x):
    high = x.astype(BF16)
    low = (x - high.astype(F32)).astype(BF16)
    return high, low


def split3(x, axis):
    high, low = split(x)
    return jnp.concatenate([high, low, high], axis=axis)


def table3(tab, which, axis):
    high = tab[which]
    return jnp.concatenate([high, high, tab[which + 1]], axis=axis)


def dot(left, right, dims):
    return lax.dot_general(left, right, (dims, ((), ())), preferred_element_type=F32)


def fill_maps(offs, vox, tcol, gathered, zmap, vmap0, vmap1):
    z = vox[0:1, :] - offs[0]
    y = vox[1:2, :] - offs[1]
    tile = tcol[...] // 16
    lane = tcol[...] % 16
    inside = (z >= 0) & (z < 16) & (y >= 0) & (y < 128)
    y = jnp.where(inside, y, -1)
    rows128 = lax.broadcasted_iota(jnp.int32, (128, SENSORS), 0)
    pick = (rows128 == tile).astype(F32).astype(BF16)
    g = gathered[...].T
    g0, g1 = split(g)
    g2 = (g - g0.astype(F32) - g1.astype(F32)).astype(BF16)
    parts = dot(jnp.concatenate([g0, g1, g2], axis=0), pick, ((1,), (0,)))
    spread = parts[0:32] + parts[32:64] + parts[64:96]
    rows16 = lax.broadcasted_iota(jnp.int32, (16, SENSORS), 0)
    here = rows16 == lane
    onrow = rows128 == y
    lhs = [jnp.where(onrow, (z + 1).astype(F32), 0.0).astype(BF16)]
    for t in range(2):
        value = jnp.sum(jnp.where(here, spread[16 * t : 16 * t + 16], 0.0), axis=0, keepdims=True)
        v0 = value.astype(BF16).astype(F32)
        v1 = (value - v0).astype(BF16).astype(F32)
        v2 = value - v0 - v1
        for part in (v0, v1, v2):
            lhs.append(jnp.where(onrow, part, 0.0).astype(BF16))
    columns = lax.broadcasted_iota(jnp.int32, (NX, SENSORS), 0)
    oncol = (columns == vox[2:3, :]).astype(F32).astype(BF16)
    out = dot(jnp.concatenate(lhs, axis=0), oncol, ((1,), (1,)))
    zmap[...] = out[0:128].astype(jnp.int32) - 1
    vmap0[...] = out[128:256] + out[256:384] + out[384:512]
    vmap1[...] = out[512:640] + out[640:768] + out[768:896]


def to_y(a, b, tab):
    return [
        dot(split3(data, 1), table3(tab, which, 0), ((1,), (0,)))
        for which, data in ((EVEN, a + b), (ODD_T, a - b))
    ]


def to_z(by_y, tab):
    by_z = []
    for x in by_y:
        top, bottom = x[:HALF], x[HALF:]
        by_z.append(dot(table3(tab, EVEN, 1), split3(top + bottom, 0), ((1,), (0,))))
        by_z.append(dot(table3(tab, ODD, 1), split3(top - bottom, 0), ((1,), (0,))))
    return by_z


def quarter(i):
    return pl.ds(i % 2 * HALF, HALF), pl.ds(i // 2 * HALF, HALF)


def forward_x(cur, tab, out):
    sums = []
    for piece in cur:
        flat = piece.reshape(PZ * 128, NX)
        sums.append((flat[:, :HALF] + flat[:, HALF:], flat[:, :HALF] - flat[:, HALF:]))
    got = [
        [dot(table3(tab, (EVEN, ODD)[part], 1), split3(pair[part], 1), ((1,), (1,))) for part in range(2)]
        for pair in sums
    ]
    for i, pair in enumerate(got):
        for part in range(2):
            pieces = [pair[part][:, z * 128 : (z + 1) * 128].reshape(64, 4, 128) for z in range(2)]
            out[pl.ds(part * 64, 64), pl.ds(i * 8, 8), :] = jnp.concatenate(pieces, axis=1)


def inverse_x(arr, tab):
    halves = []
    for i in range(ZB // PZ):
        parts = []
        for part, which in enumerate((EVEN, ODD)):
            block = arr[pl.ds(part * 64, 64), pl.ds(i * 8, 8), :]
            pieces = [block[:, z * 4 : z * 4 + 4].reshape(HALF, 128) for z in range(2)]
            data = jnp.concatenate(pieces, axis=1)
            parts.append(dot(split3(data.T, 1), table3(tab, which, 0), ((1,), (0,))))
        halves.append(parts)
    return [
        jnp.concatenate([even + odd, even - odd], axis=1).reshape(PZ, 128, NX) for even, odd in halves
    ]


def planes(i):
    return pl.ds(i * PZ, PZ)


def here(zmap, i):
    z = lax.broadcasted_iota(jnp.int32, (PZ, 1, 1), 0) + ZB * pl.program_id(0) + i * PZ
    return zmap[...][None] == z


def first_kernel(offs, vox, tcol, gathered, p, tab, zmap, vmap0, vmap1, out, p_v, sems):
    step = pl.program_id(0)

    def copy(i):
        part = pl.ds(i * ZB, ZB)
        return pltpu.make_async_copy(p.at[part], p_v.at[part], sems.at[i])

    copy(0).start()
    fill_maps(offs, vox, tcol, gathered, zmap, vmap0, vmap1)
    copy(0).wait()
    base = step * ZB
    forward_x(
        [
            jnp.where(here(zmap, i), vmap0[...][None], p_v[pl.ds(base + i * PZ, PZ)])
            for i in range(ZB // PZ)
        ],
        tab,
        out,
    )


def write_back(scratch, target, sems, i):
    group = pl.program_id(0) * (ZB // PZ) + i
    part = pl.ds(group * PZ, PZ)
    return pltpu.make_async_copy(scratch.at[part], target.at[part], sems.at[group])


def wait_all(scratch, target, sems):
    for group in range(16 // PZ):
        part = pl.ds(group * PZ, PZ)
        pltpu.make_async_copy(scratch.at[part], target.at[part], sems.at[group]).wait()


def own_planes(i):
    return pl.ds(pl.program_id(0) * ZB + i * PZ, PZ)


def middle_kernel(arr, prev, speed, p, zmap, vmap0, vmap1, tab, cur_out, out, cur_v, sems):
    current = []
    for i, update in enumerate(inverse_x(arr, tab)):
        hit = here(zmap, i)
        now = jnp.where(hit, vmap0[...][None], p[planes(i)])
        following = 2.0 * now - prev[planes(i)] + speed[planes(i)] * update
        cur = jnp.where(hit, vmap1[...][None], following)
        cur_v[own_planes(i)] = cur
        write_back(cur_v, cur_out, sems, i).start()
        current.append(cur)
    forward_x(current, tab, out)
    wait_all(cur_v, cur_out, sems)


def last_kernel(arr, cur, speed, p, zmap, vmap0, tab, final, final_v, sems):
    for i, update in enumerate(inverse_x(arr, tab)):
        before = jnp.where(here(zmap, i), vmap0[...][None], p[planes(i)])
        final_v[own_planes(i)] = 2.0 * cur[planes(i)] - before + speed[planes(i)] * update
        write_back(final_v, final, sems, i).start()
    wait_all(final_v, final, sems)


def spectral_kernel(arr, sym, tab, out):
    step = pl.program_id(0)
    by_z = analyse(arr, tab, step)
    for j in range(2):
        for i in range(4):
            rows_of, cols_of = quarter(i)
            by_z[4 * j + i] = by_z[4 * j + i] * sym[j, rows_of, cols_of]
    synthesise(by_z, tab, out, step)


def analyse(arr, tab, step):
    by_y = []
    for j in range(2):
        k = step * 2 + j
        pens = [arr[:, p, pl.ds(k, 16, stride=4), :].reshape(512, 128) for p in range(4)]
        by_y += to_y(jnp.concatenate(pens[:2], axis=1), jnp.concatenate(pens[2:], axis=1), tab)
    return to_z(by_y, tab)


def synthesise(scaled, tab, out, step):
    back_z = [
        dot(table3(tab, (EVEN, ODD_T)[i % 2], 1), split3(x, 0), ((1,), (0,)))
        for i, x in enumerate(scaled)
    ]
    back_y = []
    for part in range(4):
        even, odd = back_z[2 * part], back_z[2 * part + 1]
        z = jnp.concatenate([even + odd, even - odd], axis=0)
        back_y.append(dot(split3(z, 1), table3(tab, (EVEN, ODD)[part % 2], 0), ((1,), (0,))))
    for j in range(2):
        a = back_y[2 * j] + back_y[2 * j + 1]
        b = back_y[2 * j] - back_y[2 * j + 1]
        for p in range(4):
            piece = (a, b)[p // 2][:, (p % 2) * 128 : (p % 2) * 128 + 128]
            out[:, p, pl.ds(step * 2 + j, 16, stride=4), :] = piece.reshape(32, 16, 128)


def whole(*shape):
    return pl.BlockSpec(shape, lambda i: (0,) * len(shape))


def pairs():
    return pl.BlockSpec((ZB, 128, NX), lambda i: (i, 0, 0))


def packed():
    return pl.BlockSpec((128, 4 * ZB, 128), lambda i: (0, i, 0))


def params(mib):
    return pltpu.CompilerParams(vmem_limit_bytes=mib * MIB)


TAB = whole(6, HALF, HALF)
MAP = whole(128, NX)
WIRE = jax.ShapeDtypeStruct((128, 64, 128), F32)


def squared_freq(indices, length):
    signed_index = jnp.where(2 * indices > length, indices - length, indices)
    angular = signed_index.astype(F32) * (2.0 * math.pi / length)
    return angular * angular


def half_order(rows):
    return jnp.where(rows < HALF, 2 * rows, 2 * (rows - HALF) + 1)


def local_freq(device):
    return half_order(device * 4 + jnp.arange(4, dtype=jnp.int32))


def symbol_of(device):
    rows = jnp.arange(512, dtype=jnp.int32)
    freq = squared_freq(half_order(rows), 512)
    freq_x = squared_freq(local_freq(device), NX)
    total = freq[None, :, None] + freq[None, None, :] + freq_x[:, None, None]
    square = total * (HALF_CFL * HALF_CFL)
    ratio = jnp.full_like(square, 1.0 / math.factorial(15) * -1.0)
    for n in (13, 11, 9, 7, 5, 3, 1):
        sign = 1.0 if n % 4 == 1 else -1.0
        ratio = ratio * square + sign / math.factorial(n)
    scale = -4.0 / (NX * NY * NZ)
    return square * ratio * ratio * scale


def in_hbm(array):
    return pltpu.with_memory_space_constraint(array, pltpu.HBM)


def exchange(array):
    return lax.all_to_all(array, SLAB_PEN, split_axis=0, concat_axis=0, tiled=True)


def step_pair(pressure, previous, speed_ratio, traces, sensor_voxels, trace_column):
    slab_index = lax.axis_index(SLAB)
    pen_index = lax.axis_index("pen")
    device = slab_index * 4 + pen_index
    tab = jnp.asarray(half_tables())
    offs = jnp.stack([slab_index * 16, pen_index * 128]).astype(jnp.int32)
    gathered = exchange(jnp.broadcast_to(traces[None], (128, 2, 16)))
    sym = symbol_of(device)
    in_smem = pl.BlockSpec(memory_space=pltpu.SMEM)
    map_type = jax.ShapeDtypeStruct((128, NX), F32)
    zmap, vmap0, vmap1, wire = pl.pallas_call(
        first_kernel,
        grid=(16 // ZB,),
        in_specs=[in_smem, whole(3, SENSORS), whole(1, SENSORS), whole(128, 32), pl.BlockSpec(memory_space=pl.ANY), TAB],
        out_specs=(MAP, MAP, MAP, packed()),
        out_shape=(jax.ShapeDtypeStruct((128, NX), jnp.int32), map_type, map_type, WIRE),
        scratch_shapes=[pltpu.VMEM((16, 128, NX), F32), pltpu.SemaphoreType.DMA((16 // ZB,))],
        compiler_params=params(24),
        name="first",
    )(
        offs,
        sensor_voxels,
        trace_column.reshape(1, SENSORS),
        gathered.reshape(128, 32),
        in_hbm(pressure),
        tab,
    )
    cube = whole(32, 4, 64, 128)
    planes2 = pl.BlockSpec((2, 512, 512), lambda i: (i, 0, 0))

    def spectral(arr):
        return pl.pallas_call(
            spectral_kernel,
            grid=(2,),
            in_specs=[cube, planes2, TAB],
            out_specs=cube,
            out_shape=jax.ShapeDtypeStruct((32, 4, 64, 128), F32),
            compiler_params=params(24),
            name="spectral",
        )(arr.reshape(32, 4, 64, 128), sym, tab).reshape(128, 64, 128)

    arr = exchange(spectral(exchange(wire)))
    current, wire = pl.pallas_call(
        middle_kernel,
        grid=(16 // ZB,),
        in_specs=[packed(), pairs(), pairs(), pairs(), MAP, MAP, MAP, TAB],
        out_specs=(pl.BlockSpec(memory_space=pl.ANY), packed()),
        out_shape=(pltpu.HBM((16, 128, NX), F32), WIRE),
        scratch_shapes=[pltpu.VMEM((16, 128, NX), F32), pltpu.SemaphoreType.DMA((16 // PZ,))],
        compiler_params=params(24),
        name="middle",
    )(arr, previous, speed_ratio, pressure, zmap, vmap0, vmap1, tab)
    arr = exchange(spectral(exchange(wire)))
    final = pl.pallas_call(
        last_kernel,
        grid=(16 // ZB,),
        in_specs=[packed(), pairs(), pairs(), pairs(), MAP, MAP, TAB],
        out_specs=pl.BlockSpec(memory_space=pl.ANY),
        out_shape=pltpu.HBM((16, 128, NX), F32),
        scratch_shapes=[pltpu.VMEM((16, 128, NX), F32), pltpu.SemaphoreType.DMA((16 // PZ,))],
        compiler_params=params(24),
        name="last",
    )(arr, current, speed_ratio, pressure, zmap, vmap0, tab)
    return (final, current)


def solution(mesh):
    torus = Mesh(
        mesh.devices.reshape(4, 4, 2, mesh.shape["pen"]), ("slab_0", "slab_1", "slab_2", "pen")
    )
    placed = (
        P(SLAB, "pen", None),
        P(SLAB, "pen", None),
        P(SLAB, "pen", None),
        P(None, SLAB_PEN),
        P(),
        P(),
    )
    return jax.shard_map(
        step_pair,
        mesh=torus,
        in_specs=placed,
        out_specs=(P(SLAB, "pen", None), P(SLAB, "pen", None)),
        check_vma=False,
    )
```
